512 devices in a mesh: gx: 32 (over z, x), gy: 16 (over y, core).
Axes of the slice: x: 4, y: 8, z: 8, core: 2. Of those that a mesh axis runs over, the one named last changes fastest.
Arguments:
- gap_load: float32 [32, 16, 384, 128], P('gx', 'gy'), may hold values from -6 to 6
- flexibility: bfloat16 [32, 16, 768, 768], P('gx', 'gy'), as said below
- schur_blocks: bfloat16 [32, 16, 768, 768], P('gx', 'gy'), as said below
- body_modes: float32 [32, 16, 3, 768], P('gx', 'gy'), may hold values from -6 to 6
- coarse_inverse: float32 [1536, 1536], P(('gx', 'gy')), as said below
- saved_search: float32 [32, 16, 16, 384], P('gx', 'gy'), may hold values from -6 to 6
- saved_images: float32 [32, 16, 16, 384], P('gx', 'gy'), may hold values from -0.0017089844 to 0.0017089844
- face_slots: int32 [32, 16, 4, 192], P('gx', 'gy'), may hold values from 0 to 767, as said below
- face_count: int32 [32, 16, 4], P('gx', 'gy'), may hold values from 0 to 192, as said below
- multiplicity: int32 [32, 16, 768], P('gx', 'gy'), may hold values from 1 to 3, as said below
Outputs:
- multipliers: float32 [32, 16, 384, 128], P('gx', 'gy')
- residual: float32 [32, 16, 384, 128], P('gx', 'gy')
The draws below stay inside these ranges and needn't reach their ends.
Inputs may be any that keep to these rules, and one draw needn't show every extreme that they name: For k < face_count[a, b, d] the entries face_slots[a, b, d, k] are distinct slots of subdomain (a, b), except that faces that follow each other in the order up, right, down, left share one slot when both are not empty. Link k of the face between two neighbouring subdomains is entry k of both their lists (down of the upper one and up of the lower one, right of the left one and left of the right one). Entries with k >= face_count carry no meaning. face_count[a, b, 0] = face_count[a - 1, b, 1] and face_count[a, b, 2] = face_count[a, b - 1, 3]; faces on the grid's border have 0 links, inner faces between 96 and 192, and in every draw some face along each grid direction has exactly 192. multiplicity[a, b, i] is 1 plus the number of faces of (a, b) whose first face_count entries name slot i. `flexibility`: each block is symmetric. `schur_blocks`: each block is symmetric. `coarse_inverse`: Symmetric.
All inputs are finite; a program needn't handle non-finite values.
Results may differ from the reference program's by a relative error of at most 0.0015.
The reference program's roundings to bfloat16 on the way (of `weighted` and `lifted`) count: a program that leaves them out, or rounds other values in their place, can miss the bound.
Values sent between devices are 32-bit elements.
No kernel may reach another device: no remote copies, remote signals or barrier semaphores. Data moves between devices by JAX's collectives and lax.ppermute only.
A program may use at most 64 MiB of HBM per device.

```python
import jax
import jax.numpy as jnp
from jax import lax

NI = 768
FACE = 192
R = 128
K = 3
NDIR = 16
ITERS = 1
SX = 32
SY = 16
NC = 1536


def interface_maps(key):
    base_key = jax.random.fold_in(key, 77)
    vertical_key, horizontal_key, order_key, vertical_pick, horizontal_pick = jax.random.split(base_key, 5)
    row_index = jnp.arange(SX)[:, None]
    col_index = jnp.arange(SY)[None, :]
    vertical = jax.random.randint(vertical_key, (SX, SY), FACE // 2, FACE + 1)
    vertical = jnp.where(row_index < SX - 1, vertical, 0)
    widest = jax.random.randint(vertical_pick, (), 0, (SX - 1) * SY)
    vertical = vertical.at[widest // SY, widest % SY].set(FACE)
    horizontal = jax.random.randint(horizontal_key, (SX, SY), FACE // 2, FACE + 1)
    horizontal = jnp.where(col_index < SY - 1, horizontal, 0)
    widest_side = jax.random.randint(horizontal_pick, (), 0, SX * (SY - 1))
    horizontal = horizontal.at[widest_side // (SY - 1), widest_side % (SY - 1)].set(FACE)
    upper = jnp.concatenate([jnp.zeros((1, SY), jnp.int32), vertical[:-1]], axis=0)
    leftward = jnp.concatenate([jnp.zeros((SX, 1), jnp.int32), horizontal[:, :-1]], axis=1)
    counts = jnp.stack([upper, vertical, leftward, horizontal], axis=-1).astype(jnp.int32)
    order_keys = jax.random.split(order_key, SX * SY)
    orders = jax.vmap(lambda one_key: jax.random.permutation(one_key, NI))(order_keys).reshape(SX, SY, NI).astype(jnp.int32)
    nonempty = jnp.minimum(counts, 1)
    start_up = jnp.zeros((SX, SY), jnp.int32)
    start_right = counts[..., 0] - nonempty[..., 0] * nonempty[..., 3]
    start_down = start_right + counts[..., 3] - nonempty[..., 3] * nonempty[..., 1]
    start_left = start_down + counts[..., 1] - nonempty[..., 1] * nonempty[..., 2]
    starts = jnp.stack([start_up, start_down, start_left, start_right], axis=-1)
    position = starts[..., None] + jnp.minimum(jnp.arange(FACE, dtype=jnp.int32)[None, None, None, :], jnp.maximum(counts - 1, 0)[..., None])
    slots = jnp.take_along_axis(orders, position.reshape(SX, SY, 4 * FACE), axis=2).reshape(SX, SY, 4, FACE)
    valid = (jnp.arange(FACE)[None, None, None, :] < counts[..., None]).astype(jnp.int32)
    flat_index = (jnp.arange(SX * SY, dtype=jnp.int32)[:, None] * NI + slots.reshape(SX * SY, 4 * FACE)).reshape(-1)
    shared = jnp.zeros((SX * SY * NI,), jnp.int32).at[flat_index].add(valid.reshape(-1))
    return (slots.astype(jnp.int32), counts, (1 + shared).reshape(SX, SY, NI))


def draw_face_slots(key, part):
    return interface_maps(key)[0]


def draw_face_count(key, part):
    return interface_maps(key)[1]


def draw_multiplicity(key, part):
    return interface_maps(key)[2]


def symmetric_blocks(key, fold_tag):
    base_key = jax.random.fold_in(key, fold_tag)
    factor = 1.0 / (2.0 * jnp.sqrt(2.0 * NI))

    def one_row(row):
        row_key = jax.random.fold_in(base_key, row)
        noise_draw = jax.random.normal(row_key, (SY, NI, NI), jnp.float32)
        noise_draw = (noise_draw + jnp.swapaxes(noise_draw, 1, 2)) * factor
        return (2.0 * jnp.eye(NI, dtype=jnp.float32) + noise_draw).astype(jnp.bfloat16)
    return lax.map(one_row, jnp.arange(SX))


def draw_flexibility(key, part):
    return symmetric_blocks(key, 11)


def draw_schur_blocks(key, part):
    return symmetric_blocks(key, 12)


def draw_coarse_inverse(key, part):
    noise_key = jax.random.fold_in(key, 31)
    noise_draw = jax.random.normal(noise_key, (NC, NC), jnp.float32)
    factor = 0.3 / jnp.sqrt(2.0 * NC)
    return (jnp.eye(NC, dtype=jnp.float32) + factor * (noise_draw + noise_draw.T)) * (3.0 / NI)


def block_scale(own_key, dims, shards, smallest, largest):
    def one(axis_at, shards_of):
        steps = jax.random.uniform(jax.random.fold_in(jax.random.fold_in(own_key, 6), axis_at), (shards_of,), jnp.float32, smallest / len(shards), largest / len(shards))
        return jnp.repeat(jnp.exp(steps), dims[axis_at] // shards_of).reshape((-1,) + (1,) * (len(dims) - axis_at - 1))

    factor_of = one(*shards[0])
    for cut in shards[1:]:
        factor_of = factor_of * one(*cut)
    return factor_of


def scatter_about(stream_key, shape, deviation, reach, shards=(), kind=jnp.bfloat16):
    array = jax.random.normal(stream_key, shape, jnp.float32) * deviation
    if len(shards) > 0:
        array = block_scale(stream_key, shape, shards, -0.22, 0.18) * array
    return jnp.clip(array, min=-reach, max=reach).astype(kind)


def setup_inputs(seed: int = 0) -> dict:
    keys = jax.random.split(jax.random.key(seed), 11)
    gap_load = scatter_about(keys[0], (SX, SY, 2 * FACE, R), 1.0, 6.0, ((0, 32), (1, 16)), jnp.float32)
    flexibility = draw_flexibility(jax.random.fold_in(keys[10], 71), 0)
    schur_blocks = draw_schur_blocks(jax.random.fold_in(keys[10], 71), 0)
    body_modes = scatter_about(keys[3], (SX, SY, K, NI), 1.0, 6.0, ((0, 32), (1, 16)), jnp.float32)
    coarse_inverse = draw_coarse_inverse(jax.random.fold_in(keys[10], 71), 0)
    saved_search = scatter_about(keys[5], (SX, SY, NDIR, 2 * FACE), 1.0, 6.0, ((0, 32), (1, 16)), jnp.float32)
    saved_images = scatter_about(keys[6], (SX, SY, NDIR, 2 * FACE), (8 * FACE * SX * SY * NDIR) ** -0.5, 0.0017089844, ((0, 32), (1, 16)), jnp.float32)
    face_slots = draw_face_slots(jax.random.fold_in(keys[10], 71), 0)
    face_count = draw_face_count(jax.random.fold_in(keys[10], 71), 0)
    multiplicity = draw_multiplicity(jax.random.fold_in(keys[10], 71), 0)
    return dict(gap_load=gap_load, flexibility=flexibility, schur_blocks=schur_blocks, body_modes=body_modes, coarse_inverse=coarse_inverse, saved_search=saved_search, saved_images=saved_images, face_slots=face_slots, face_count=face_count, multiplicity=multiplicity)


HIGHEST_MODE = lax.Precision.HIGHEST


def spread(link_values, face_slots, face_valid):
    load_cases = link_values.shape[-1]
    down_links = link_values[:, :, :FACE]
    right_links = link_values[:, :, FACE:]
    from_above = jnp.concatenate([jnp.zeros_like(down_links[:1]), down_links[:-1]], axis=0)
    from_left = jnp.concatenate([jnp.zeros_like(right_links[:, :1]), right_links[:, :-1]], axis=1)
    signed_parts = jnp.stack([-from_above, down_links, -from_left, right_links], axis=2) * face_valid[..., None]

    def deposit(slot_rows, values):
        empty = jnp.zeros((NI, load_cases), values.dtype)
        return empty.at[slot_rows.reshape(-1)].add(values.reshape(-1, load_cases))

    return jax.vmap(jax.vmap(deposit))(face_slots, signed_parts)


def jumps(slot_values, face_slots, face_valid):
    load_cases = slot_values.shape[-1]

    def select(values, slot_rows):
        return values[slot_rows.reshape(-1)]

    picked = jax.vmap(jax.vmap(select))(slot_values, face_slots).reshape(SX, SY, 4, FACE, load_cases)
    from_below = jnp.concatenate([picked[1:, :, 0], jnp.zeros_like(picked[:1, :, 0])], axis=0)
    from_right = jnp.concatenate([picked[:, 1:, 2], jnp.zeros_like(picked[:, :1, 2])], axis=1)
    down_part = (picked[:, :, 1] - from_below) * face_valid[:, :, 1, :, None]
    right_part = (picked[:, :, 3] - from_right) * face_valid[:, :, 3, :, None]
    return jnp.concatenate([down_part, right_part], axis=2)


def blockwise(matrices, vectors):
    def row_block(operands):
        return jnp.einsum("bij,bjc->bic", operands[0].astype(jnp.float32), operands[1].astype(jnp.float32), precision=HIGHEST_MODE)

    return lax.map(row_block, (matrices, vectors))


def reference(gap_load, flexibility, schur_blocks, body_modes, coarse_inverse, saved_search, saved_images, face_slots, face_count, multiplicity):
    face_valid = (jnp.arange(FACE)[None, None, None, :] < face_count[..., None]).astype(jnp.float32)
    link_valid = jnp.concatenate([face_valid[:, :, 1], face_valid[:, :, 3]], axis=2)
    weights = 1.0 / multiplicity.astype(jnp.float32)
    residual = gap_load * link_valid[..., None]
    kept_search = saved_search * link_valid[:, :, None, :]
    kept_images = saved_images * link_valid[:, :, None, :]
    multipliers = jnp.zeros_like(residual)
    search_before = residual
    energy_before = jnp.ones((R,), jnp.float32)
    for iteration in range(ITERS):
        weighted = (weights[..., None] * spread(residual, face_slots, face_valid)).astype(jnp.bfloat16)
        smoothed = blockwise(schur_blocks, weighted)
        precond = jumps(weights[..., None] * smoothed, face_slots, face_valid)
        energy = jnp.sum(residual * precond, axis=(0, 1, 2))
        coarse_in = jnp.einsum("abki,abic->abkc", body_modes, spread(precond, face_slots, face_valid), precision=HIGHEST_MODE)
        coarse_out = jnp.dot(coarse_inverse, coarse_in.reshape(NC, R), precision=HIGHEST_MODE).reshape(SX, SY, K, R)
        lifted_modes = jnp.einsum("abki,abkc->abic", body_modes, coarse_out, precision=HIGHEST_MODE)
        projected = precond - jumps(lifted_modes, face_slots, face_valid)
        intersect = jnp.einsum("abjl,ablc->jc", kept_images, projected, precision=HIGHEST_MODE)
        search = projected - jnp.einsum("abjl,jc->ablc", kept_search, intersect, precision=HIGHEST_MODE)
        if iteration > 0:
            search = search + (energy / energy_before) * search_before
        lifted = spread(search, face_slots, face_valid).astype(jnp.bfloat16)
        applied = jumps(blockwise(flexibility, lifted), face_slots, face_valid)
        curvature = jnp.sum(search * applied, axis=(0, 1, 2))
        step_size = energy / curvature
        multipliers = multipliers + step_size * search
        residual = residual - step_size * applied
        search_before = search
        energy_before = energy
    return multipliers, residual
```

```python
import functools

import jax
import jax.numpy as jnp
import numpy as np
from jax import lax
from jax.experimental import pallas as pl
from jax.experimental.pallas import tpu as pltpu
from jax.sharding import Mesh
from jax.sharding import PartitionSpec as P

GX = ("gx_0", "gx_1")
GY = ("gy_0", "gy_1")
GX_GY = ("gx_0", "gx_1", "gy_0", "gy_1")

F32 = jnp.float32
BF16 = jnp.bfloat16
HIGHEST = lax.Precision.HIGHEST
SIGNS = (-1.0, 1.0, -1.0, 1.0)


def shifted(value, axis, steps):
    count = lax.axis_size(axis)
    initial, last = (max(0, -steps), min(count, count - steps))
    return lax.ppermute(value, axis, [(source, source + steps) for source in range(initial, last)])


def split3(x):
    high = x.astype(BF16)
    rest = x - high.astype(F32)
    mid = rest.astype(BF16)
    low = (rest - mid.astype(F32)).astype(BF16)
    return high, mid, low


def dot(a, b):
    return lax.dot_general(a, b, (((1,), (0,)), ((), ())), preferred_element_type=F32)


def dot_nt(a, b):
    return lax.dot_general(a, b, (((1,), (1,)), ((), ())), preferred_element_type=F32)


def dot_exact(a, b):
    return lax.dot_general(
        a, b, (((1,), (0,)), ((), ())), precision=HIGHEST, preferred_element_type=F32
    )


def select_rows(selection, x):
    width = x.shape[1]
    out = dot(selection, jnp.concatenate(split3(x), axis=1))
    return out[:, :width] + (out[:, width : 2 * width] + out[:, 2 * width :])


def select_lanes(x, selection):
    rows = x.shape[0]
    out = dot(jnp.concatenate(split3(x), axis=0), selection)
    return out[:rows] + (out[rows : 2 * rows] + out[2 * rows :])


def six_left(tiled):
    high, mid, low = split3(tiled)
    group = lax.broadcasted_iota(jnp.int32, tiled.shape, 1) // 16
    zero = jnp.zeros_like(tiled)
    is_high = (group == 0) | (group == 1) | (group == 3)
    is_mid = (group == 2) | (group == 4)
    out = jnp.where(
        is_high,
        high.astype(F32),
        jnp.where(is_mid, mid.astype(F32), jnp.where(group == 5, low.astype(F32), zero)),
    )
    return out.astype(BF16)


def six_right(x):
    high, mid, low = split3(x)
    zero = jnp.zeros_like(high)
    return jnp.concatenate([high, mid, high, low, mid, high, zero, zero], axis=0)


def tile_matrix():
    row = lax.broadcasted_iota(jnp.int32, (16, 128), 0)
    lane = lax.broadcasted_iota(jnp.int32, (16, 128), 1)
    return jnp.where(lane % 16 == row, 1.0, 0.0).astype(F32)


def widened(x, lanes):
    return jnp.concatenate([x, jnp.zeros((x.shape[0], lanes - x.shape[1]), x.dtype)], axis=1)


def lane_window(x, start, width):
    total = x.shape[1]
    if start:
        x = pltpu.roll(x, total - start, 1)
    return x[:, :width]


def at_lanes(x, start):
    return pltpu.roll(x, start, 1) if start else x


def prepare_kernel(
    windows, count, slots, mult, modes, schur, coarse,
    place, pick, pick_schur, mode_rows, mode_cols, columns, blocks, buffer, wide,
):
    width = slots.shape[1]
    total = 4 * width
    buffer[...] = jnp.zeros_like(buffer)
    buffer[0:4, 0:width] = slots[...].astype(F32)
    raw = buffer[...]
    lane = lax.broadcasted_iota(jnp.int32, (1, total), 1)
    slot_row = jnp.zeros((1, total), F32)
    sign_row = jnp.zeros((1, total), F32)
    for f in range(4):
        inside = (lane >= width * f) & (lane < width * f + count[f])
        slot_row = jnp.where(inside, at_lanes(raw, width * f)[f : f + 1], slot_row)
        sign_row = jnp.where(inside, SIGNS[f], sign_row)
    weights = 1.0 / mult[...].astype(F32)
    buffer[...] = jnp.zeros_like(buffer)
    buffer[0:1, :] = slot_row
    buffer[1:2, :] = sign_row
    buffer[2:3, :] = weights
    cols = jnp.transpose(buffer[...])
    columns[...] = cols
    down = lax.broadcasted_iota(jnp.int32, (total, total), 0).astype(F32)
    place_value = jnp.where(down == slot_row, sign_row, 0.0).astype(BF16)
    place[...] = place_value
    across = lax.broadcasted_iota(jnp.int32, (total, total), 1).astype(F32)
    pick_value = jnp.where(across == cols[:, 0:1], cols[:, 1:2], 0.0).astype(BF16)
    pick[...] = pick_value
    buffer[...] = jnp.zeros_like(buffer)
    buffer[0:3, :] = modes[...]
    buffer[3:4, :] = weights
    rows = select_lanes(buffer[...], place_value)
    mode_rows[...] = rows
    mode_cols[...] = jnp.transpose(rows)
    pick_schur[...] = dot(pick_value, schur[...]).astype(BF16)
    wide[...] = jnp.zeros_like(wide)
    wide[0:3, :] = coarse[...]
    for i, start in enumerate(windows):
        blocks[8 * i : 8 * i + 8, :] = wide[:, start : start + blocks.shape[1]]


def precond_kernel(
    gap, above, left, place, pick_schur, columns, mode_rows, mode_cols, saved,
    up_msg, down_msg, left_msg, right_msg, own,
):
    width = above.shape[0]
    links = jnp.concatenate([above[...], gap[0:width], left[...], gap[width:]], axis=0)
    spread = select_rows(place[...], links)
    weighted = (columns[:, 2:3] * spread).astype(BF16)
    picked = jnp.abs(mode_cols[:, 3:4]) * dot(pick_schur[...], weighted)
    own[...] = picked
    for f, msg in enumerate((up_msg, down_msg, left_msg, right_msg)):
        msg[0:width, :] = picked[width * f : width * f + width]
        rows = lane_window(mode_rows[...], width * f, 256)
        msg[width : width + 8, :] = rows[:, 0:128]
        msg[width + 8 : width + 16, :] = rows[:, 128:256]
    for start, msg in ((0, down_msg), (width, right_msg)):
        rows = lane_window(saved[...], start, 256)
        msg[width + 16 : width + 32, :] = rows[:, 0:128]
        msg[width + 32 : width + 48, :] = rows[:, 128:256]


def flex_kernel(pick, place, flex, pick_flex, link_flex):
    rows = dot(pick[...], flex[...]).astype(BF16)
    pick_flex[...] = rows
    link_flex[...] = dot(rows, place[...]).astype(BF16)


def coarse_in_kernel(own, above, below, left, right, mode_rows, precond, coarse):
    width = own.shape[0] // 4
    full = own[...] + jnp.concatenate(
        [above[0:width], below[0:width], left[0:width], right[0:width]], axis=0
    )
    precond[...] = full
    rows = dot_exact(mode_rows[...], full)
    rows = jnp.where(lax.broadcasted_iota(jnp.int32, rows.shape, 0) < 3, rows, 0.0)
    for i in range(coarse.shape[0] // 8):
        coarse[8 * i : 8 * i + 8, :] = rows


def tables_kernel(
    count, offset, above, below, left, right, mode_rows, saved, images, link_flex, gap, precond,
    blocks, wanted,
    mode_six, search_six, forms, sums, coarse_rows,
):
    total = mode_rows.shape[1]
    width = total // 4
    tiles = tile_matrix()
    lane = lax.broadcasted_iota(jnp.int32, (1, 256), 1)
    row = lax.broadcasted_iota(jnp.int32, (16, total), 0)
    mine = jnp.concatenate([mode_rows[...], jnp.zeros((8, total), F32)], axis=0)
    modes = jnp.where(row < 3, mine, 0.0)
    for f, msg in enumerate((above, below, left, right)):
        theirs = jnp.concatenate([msg[width : width + 8], msg[width + 8 : width + 16]], axis=1)
        theirs = jnp.where(lane < count[f], theirs, 0.0)
        theirs = at_lanes(widened(theirs, total), width * f)
        theirs = jnp.concatenate([theirs, jnp.zeros((8, total), F32)], axis=0)
        theirs = jnp.where(row < 3, theirs, 0.0)
        modes = modes + pltpu.roll(theirs, 3 * (1 + f), 0)
    mode_six[...] = six_left(
        lax.dot_general(modes, tiles, (((0,), (0,)), ((), ())), precision=HIGHEST, preferred_element_type=F32)
    )
    search = jnp.zeros((16, total), F32)
    for f in range(4):
        if f % 2 == 0:
            msg = above if f == 0 else left
            piece = jnp.concatenate(
                [msg[width + 16 : width + 32], msg[width + 32 : width + 48]], axis=1
            )
        else:
            piece = lane_window(saved[...], 0 if f == 1 else width, 256)
        piece = jnp.where(lane < count[f], piece, 0.0)
        search = search + at_lanes(widened(piece, total), width * f)
    search_tiled = lax.dot_general(
        search, tiles, (((0,), (0,)), ((), ())), precision=HIGHEST, preferred_element_type=F32
    )
    search_six[...] = six_left(search_tiled)
    flex_search = select_lanes(search, link_flex[...])
    lanes = lax.broadcasted_iota(jnp.int32, (16, total), 1)
    image = widened(images[...], total)
    image_down = at_lanes(image, width)
    image_right = at_lanes(image, 2 * width)
    forms[0:16, :] = jnp.where(
        (lanes >= width) & (lanes < 2 * width),
        image_down,
        jnp.where(lanes >= 3 * width, image_right, 0.0),
    )
    forms[16:32, :] = flex_search
    products = dot_exact(flex_search, search_tiled)
    group = lax.broadcasted_iota(jnp.int32, (16, 128), 1) // 16
    part = lax.broadcasted_iota(jnp.int32, (16, 128), 0)
    products = jnp.where(group == part % 8, products, 0.0)
    energy = jnp.sum(gap[0:width] * precond[width : 2 * width], axis=0, keepdims=True) + jnp.sum(
        gap[width:] * precond[3 * width :], axis=0, keepdims=True
    )
    sums[...] = jnp.concatenate(
        [
            energy,
            jnp.zeros((1, 128), F32),
            jnp.sum(products[0:8], axis=0, keepdims=True),
            jnp.sum(products[8:16], axis=0, keepdims=True),
            jnp.zeros((4, 128), F32),
        ],
        axis=0,
    )
    at = lax.broadcasted_iota(jnp.int32, (wanted.shape[0], blocks.shape[1]), 1)
    chosen = jnp.where(at == wanted[:, 0:1] + offset[0], 1.0, 0.0).astype(BF16)
    high, mid, low = split3(blocks[...])
    coarse_rows[...] = dot_nt(chosen, high) + (dot_nt(chosen, mid) + dot_nt(chosen, low))


def coarse_kernel(coarse_rows, gathered, parts):
    parts[...] = dot_exact(coarse_rows[...], gathered[...])


def project_kernel(arrived, precond, mode_six, forms, sums, link_flex, projected, partial):
    amplitudes = arrived[0:16]
    for j in range(1, arrived.shape[0] // 16):
        amplitudes = amplitudes + arrived[16 * j : 16 * j + 16]
    links = precond[...] - dot(mode_six[...], six_right(amplitudes))
    projected[...] = links
    linear = dot_exact(forms[...], links)
    high, mid, _ = split3(links)
    image = dot(link_flex[...], jnp.concatenate([high, mid], axis=1))
    square = jnp.sum(links * (image[:, :128] + image[:, 128:]), axis=0, keepdims=True)
    row = lax.broadcasted_iota(jnp.int32, (8, 128), 0)
    last = jnp.where(row == 1, square, sums[...])
    for j in range(partial.shape[0] // 40):
        partial[40 * j : 40 * j + 32, :] = linear
        partial[40 * j + 32 : 40 * j + 40, :] = last


def block_sum(ref, height):
    out = ref[0:height]
    for j in range(1, ref.shape[0] // height):
        out = out + ref[height * j : height * j + height]
    return out


def spread_sum_kernel(arrived, partial):
    out = block_sum(arrived, 40)
    for i in range(partial.shape[0] // 40):
        partial[40 * i : 40 * i + 40, :] = out


def search_kernel(
    arrived, projected, search_six, place, pick_flex,
    up_msg, left_msg, own, multipliers, step,
):
    width = up_msg.shape[0]
    sums = block_sum(arrived, 40)
    intersect = sums[0:16]
    cross = sums[16:32]
    energy = sums[32:33]
    square = sums[33:34]
    group = lax.broadcasted_iota(jnp.int32, (16, 128), 1) // 16
    part = lax.broadcasted_iota(jnp.int32, (16, 128), 0)
    packed = jnp.where(part < 8, sums[34:35], sums[35:36])
    packed = jnp.where(group == part % 8, packed, 0.0)
    products = dot_exact(packed, jnp.concatenate([intersect] * 8, axis=0))
    curvature = square + jnp.sum(intersect * (products - 2.0 * cross), axis=0, keepdims=True)
    size = energy / curvature
    step[...] = jnp.broadcast_to(size, step.shape)
    search = projected[...] - dot(search_six[...], six_right(intersect))
    multipliers[0:width, :] = size * search[width : 2 * width]
    multipliers[width:, :] = size * search[3 * width :]
    lifted = select_rows(place[...], search).astype(BF16)
    image = dot(pick_flex[...], lifted)
    up_msg[...] = image[0:width]
    own[0:width, :] = image[width : 2 * width]
    left_msg[...] = image[2 * width : 3 * width]
    own[width:, :] = image[3 * width :]


def residual_kernel(count, gap, own, below, right, step, residual):
    width = below.shape[0]
    row = lax.broadcasted_iota(jnp.int32, below.shape, 0)
    size = step[0:1]
    residual[0:width, :] = jnp.where(
        row < count[1], gap[0:width] - size * (own[0:width] + below[...]), 0.0
    )
    residual[width:, :] = jnp.where(
        row < count[3], gap[width:] - size * (own[width:] + right[...]), 0.0
    )


VMEM_LIMIT = 24 * 1024 * 1024
VMEM = pl.BlockSpec(memory_space=pltpu.VMEM)
SMEM = pl.BlockSpec(memory_space=pltpu.SMEM)


def call(kernel, inputs, outputs, scalars=0, scratch=(), flops=0, name=None):
    outputs = tuple(jax.ShapeDtypeStruct(shape, dtype) for shape, dtype in outputs)
    return pl.pallas_call(
        kernel,
        out_shape=outputs,
        in_specs=[SMEM] * scalars + [VMEM] * (len(inputs) - scalars),
        out_specs=tuple(VMEM for _ in outputs),
        scratch_shapes=[pltpu.VMEM(shape, dtype) for shape, dtype in scratch],
        cost_estimate=pl.CostEstimate(flops=flops, transcendentals=0, bytes_accessed=0),
        compiler_params=pltpu.CompilerParams(vmem_limit_bytes=VMEM_LIMIT),
        name=name,
    )(*inputs)


def wanted_rows(columns, modes):
    table = np.full((columns * 16, 128), -(1 << 20), np.int32)
    for j in range(columns):
        for s, (down, right) in enumerate(((0, 0), (-1, 0), (1, 0), (0, -1), (0, 1))):
            if 0 <= j + right < columns:
                for k in range(modes):
                    table[16 * j + modes * s + k] = ((down + 1) * columns + j + right) * modes + k
    return table


def per_device(
    gap_load, flexibility, schur_blocks, body_modes, coarse_inverse,
    saved_search, saved_images, face_slots, face_count, multiplicity,
):
    rows = lax.axis_size(GX)
    columns = lax.axis_size(GY)
    gap = gap_load[0, 0]
    flex = flexibility[0, 0]
    modes = body_modes[0, 0]
    saved = saved_search[0, 0]
    images = saved_images[0, 0]
    slots = face_slots[0, 0]
    count = face_count[0, 0]
    width = slots.shape[1]
    total = 4 * width
    cases = gap.shape[1]
    unknowns = coarse_inverse.shape[1]
    row_unknowns = columns * modes.shape[0]
    window = min(unknowns, 384)
    windows = [
        min(max((row_unknowns * (i - 1)) // 128, 0), (unknowns - window) // 128) * 128
        for i in range(rows)
    ]
    here = lax.axis_index(GX)
    offsets = jnp.asarray([row_unknowns * (i - 1) - windows[i] for i in range(rows)], jnp.int32)
    offset = lax.dynamic_slice(offsets, (here,), (1,))

    above = shifted(gap[:width], GX, 1)
    left = shifted(gap[width:], GY, 1)
    big = (total, total)
    cube = 2 * total**3
    place, pick, pick_schur, mode_rows, mode_cols, slot_cols, blocks = call(
        functools.partial(prepare_kernel, windows),
        (count, slots, multiplicity[0], modes, schur_blocks[0, 0], coarse_inverse),
        (
            (big, BF16), (big, BF16), (big, BF16), ((8, total), F32), ((total, 8), F32),
            ((total, 8), F32), ((8 * rows, window), F32),
        ),
        scalars=1,
        scratch=(((8, total), F32), ((8, unknowns), F32)),
        flops=cube,
        name="prepare",
    )
    blocks = lax.all_to_all(blocks, GX, 0, 0, tiled=True)
    up_msg, down_msg, left_msg, right_msg, own = call(
        precond_kernel,
        (gap, above, left, place, pick_schur, slot_cols, mode_rows, mode_cols, saved),
        tuple(((width + extra, cases), F32) for extra in (16, 48, 16, 48)) + (((total, cases), F32),),
        flops=cube // 2,
        name="precond",
    )
    from_above = shifted(down_msg, GX, 1)
    from_below = shifted(up_msg, GX, -1)
    from_left = shifted(right_msg, GY, 1)
    from_right = shifted(left_msg, GY, -1)
    pick_flex, link_flex = call(
        flex_kernel, (pick, place, flex), ((big, BF16), (big, BF16)), flops=2 * cube, name="flex"
    )
    precond, coarse_in = call(
        coarse_in_kernel,
        (own, from_above, from_below, from_left, from_right, mode_rows),
        (((total, cases), F32), ((8 * rows, cases), F32)),
        flops=cube // 16,
        name="coarse_in",
    )
    gathered = lax.all_to_all(coarse_in, GX, 0, 0, tiled=True)
    mode_six, search_six, forms, sums, coarse_rows = call(
        tables_kernel,
        (
            count, offset, from_above, from_below, from_left, from_right, mode_rows, saved, images,
            link_flex, gap, precond, blocks, jnp.asarray(wanted_rows(columns, modes.shape[0])),
        ),
        (
            ((total, 128), BF16), ((total, 128), BF16), ((32, total), F32), ((8, cases), F32),
            ((16 * columns, 8 * rows), F32),
        ),
        scalars=2,
        flops=cube,
        name="tables",
    )
    (parts,) = call(
        coarse_kernel, (coarse_rows, gathered), (((16 * columns, cases), F32),), flops=cube // 8,
        name="coarse",
    )
    parts = lax.all_to_all(parts, GY, 0, 0, tiled=True)
    projected, partial = call(
        project_kernel,
        (parts, precond, mode_six, forms, sums, link_flex),
        (((total, cases), F32), ((40 * columns, cases), F32)),
        flops=cube // 2,
        name="project",
    )
    partial = lax.all_to_all(partial, GY, 0, 0, tiled=True)
    (partial,) = call(
        spread_sum_kernel, (partial,), (((40 * rows, cases), F32),), flops=cube // 16, name="spread_sum"
    )
    partial = lax.all_to_all(partial, GX, 0, 0, tiled=True)
    up_msg, left_msg, own, multipliers, step = call(
        search_kernel,
        (partial, projected, search_six, place, pick_flex),
        (
            ((width, cases), F32), ((width, cases), F32), ((2 * width, cases), F32),
            ((2 * width, cases), F32), ((8, cases), F32),
        ),
        flops=cube // 2,
        name="search",
    )
    from_below = shifted(up_msg, GX, -1)
    from_right = shifted(left_msg, GY, -1)
    (residual,) = call(
        residual_kernel,
        (count, gap, own, from_below, from_right, step),
        (((2 * width, cases), F32),),
        scalars=1,
        flops=cube // 64,
        name="residual",
    )
    return (multipliers[None, None], residual[None, None])


def split_shape(mesh):
    rows, columns = (mesh.devices.shape[0], mesh.devices.shape[1])
    inner = 4 if rows % 4 == 0 and rows > 4 else 2
    return (rows // inner, inner, columns // 2, 2)


def solution(mesh):
    split = Mesh(mesh.devices.reshape(split_shape(mesh)), GX_GY)
    placed = (
        P(GX, GY, None, None),
        P(GX, GY, None, None),
        P(GX, GY, None, None),
        P(GX, GY, None, None),
        P(GX_GY, None),
        P(GX, GY, None, None),
        P(GX, GY, None, None),
        P(GX, GY, None, None),
        P(GX, GY, None),
        P(GX, GY, None),
    )
    return jax.shard_map(
        per_device,
        mesh=split,
        in_specs=placed,
        out_specs=(P(GX, GY, None, None), P(GX, GY, None, None)),
        check_vma=False,
    )
```

```python
import functools

import jax
import jax.numpy as jnp
from jax import lax
from jax.experimental import pallas as pl
from jax.experimental.pallas import tpu as pltpu
from jax.sharding import Mesh
from jax.sharding import PartitionSpec as P


GX = ("gx_0", "gx_1")
GY = ("gy_0", "gy_1")
GX_GY = ("gx_0", "gx_1", "gy_0", "gy_1")

F32 = jnp.float32
BF16 = jnp.bfloat16
HIGHEST = lax.Precision.HIGHEST
SIGNS = (-1.0, 1.0, -1.0, 1.0)


def shifted(value, axis, steps):
    count = lax.axis_size(axis)
    initial, last = (max(0, -steps), min(count, count - steps))
    return lax.ppermute(value, axis, [(source, source + steps) for source in range(initial, last)])


def split3(x):
    high = x.astype(BF16)
    rest = x - high.astype(F32)
    mid = rest.astype(BF16)
    low = (rest - mid.astype(F32)).astype(BF16)
    return high, mid, low


def dot(a, b):
    return lax.dot_general(a, b, (((1,), (0,)), ((), ())), preferred_element_type=F32)


def dot_nt(a, b):
    return lax.dot_general(a, b, (((1,), (1,)), ((), ())), preferred_element_type=F32)


def dot_exact(a, b):
    return lax.dot_general(
        a, b, (((1,), (0,)), ((), ())), precision=HIGHEST, preferred_element_type=F32
    )


def select_rows(selection, x):
    width = x.shape[1]
    out = dot(selection, jnp.concatenate(split3(x), axis=1))
    return out[:, :width] + (out[:, width : 2 * width] + out[:, 2 * width :])


def select_lanes(x, selection):
    rows = x.shape[0]
    out = dot(jnp.concatenate(split3(x), axis=0), selection)
    return out[:rows] + (out[rows : 2 * rows] + out[2 * rows :])


def six_left(tiled):
    high, mid, low = split3(tiled)
    group = lax.broadcasted_iota(jnp.int32, tiled.shape, 1) // 16
    zero = jnp.zeros_like(tiled)
    is_high = (group == 0) | (group == 1) | (group == 3)
    is_mid = (group == 2) | (group == 4)
    out = jnp.where(
        is_high,
        high.astype(F32),
        jnp.where(is_mid, mid.astype(F32), jnp.where(group == 5, low.astype(F32), zero)),
    )
    return out.astype(BF16)


def six_right(x):
    high, mid, low = split3(x)
    zero = jnp.zeros_like(high)
    return jnp.concatenate([high, mid, high, low, mid, high, zero, zero], axis=0)


def tile_matrix():
    row = lax.broadcasted_iota(jnp.int32, (16, 128), 0)
    lane = lax.broadcasted_iota(jnp.int32, (16, 128), 1)
    return jnp.where(lane % 16 == row, 1.0, 0.0).astype(F32)


def widened(x, lanes):
    return jnp.concatenate([x, jnp.zeros((x.shape[0], lanes - x.shape[1]), x.dtype)], axis=1)


def lane_window(x, start, width):
    total = x.shape[1]
    if start:
        x = pltpu.roll(x, total - start, 1)
    return x[:, :width]


def at_lanes(x, start):
    return pltpu.roll(x, start, 1) if start else x


def first_kernel(windows, gap_hbm, coarse_hbm, down, right, blocks, coarse, wide, arrived):
    width = down.shape[0]
    copies = [
        pltpu.make_async_copy(source, target, arrived.at[n])
        for n, (source, target) in enumerate(
            (
                (coarse_hbm, coarse),
                (gap_hbm.at[pl.ds(0, width)], down),
                (gap_hbm.at[pl.ds(width, width)], right),
            )
        )
    ]
    for copy in copies:
        copy.start()
    wide[...] = jnp.zeros_like(wide)
    copies[0].wait()
    wide[0:3, :] = coarse[...]
    for i, start in enumerate(windows):
        blocks[8 * i : 8 * i + 8, :] = wide[:, start : start + blocks.shape[1]]
    copies[1].wait()
    copies[2].wait()


def prepare_kernel(
    count_hbm, slots_hbm, mult_hbm, modes_hbm, schur_hbm,
    place, pick_schur, mode_rows, link_rows, columns,
    buffer, slots, mult, modes, schur, count, arrived,
):
    copies = [
        pltpu.make_async_copy(source, target, arrived.at[n])
        for n, (source, target) in enumerate(
            (
                (count_hbm, count), (slots_hbm, slots), (mult_hbm, mult), (modes_hbm, modes),
                (schur_hbm, schur),
            )
        )
    ]
    for copy in copies:
        copy.start()
    width = slots.shape[1]
    total = 4 * width
    buffer[...] = jnp.zeros_like(buffer)
    lane = lax.broadcasted_iota(jnp.int32, (1, total), 1)
    copies[0].wait()
    copies[1].wait()
    buffer[0:4, 0:width] = slots[...].astype(F32)
    raw = buffer[...]
    slot_row = jnp.zeros((1, total), F32)
    sign_row = jnp.zeros((1, total), F32)
    for f in range(4):
        inside = (lane >= width * f) & (lane < width * f + count[0, f])
        slot_row = jnp.where(inside, at_lanes(raw, width * f)[f : f + 1], slot_row)
        sign_row = jnp.where(inside, SIGNS[f], sign_row)
    copies[2].wait()
    weights = 1.0 / mult[...].astype(F32)
    down = lax.broadcasted_iota(jnp.int32, (total, total), 0).astype(F32)
    place_value = jnp.where(down == slot_row, sign_row, 0.0).astype(BF16)
    place[...] = place_value
    copies[3].wait()
    buffer[...] = jnp.zeros_like(buffer)
    for k in range(modes.shape[0]):
        buffer[k : k + 1, :] = modes[k]
    buffer[3:4, :] = weights
    rows = select_lanes(buffer[...], place_value)
    mode_rows[...] = rows
    buffer[...] = jnp.zeros_like(buffer)
    buffer[0:1, :] = slot_row
    buffer[1:2, :] = sign_row
    buffer[2:3, :] = weights
    buffer[3:4, :] = jnp.abs(rows[3:4])
    link_rows[...] = buffer[...]
    cols = jnp.transpose(buffer[...])
    columns[...] = cols
    pick_value = picking(cols)
    copies[4].wait()
    pick_schur[...] = dot(pick_value, schur[...]).astype(BF16)


def picking(cols):
    total = cols.shape[0]
    across = lax.broadcasted_iota(jnp.int32, (total, total), 1).astype(F32)
    return jnp.where(across == cols[:, 0:1], cols[:, 1:2], 0.0).astype(BF16)


def precond_kernel(
    gap_down, gap_right, above, left, place, pick_schur, columns, mode_rows, saved,
    up_msg, down_msg, left_msg, right_msg, own, residual,
):
    width = above.shape[0]
    links = jnp.concatenate([above[...], gap_down[...], left[...], gap_right[...]], axis=0)
    spread = select_rows(place[...], links)
    weighted = (columns[:, 2:3] * spread).astype(BF16)
    picked = columns[:, 3:4] * dot(pick_schur[...], weighted)
    own[...] = picked
    for f, msg in enumerate((up_msg, down_msg, left_msg, right_msg)):
        msg[0:width, :] = picked[width * f : width * f + width]
        rows = lane_window(mode_rows[...], width * f, 256)
        msg[width : width + 8, :] = rows[:, 0:128]
        msg[width + 8 : width + 16, :] = rows[:, 128:256]
    for start, msg in ((0, down_msg), (width, right_msg)):
        rows = lane_window(saved[...], start, 256)
        msg[width + 16 : width + 32, :] = rows[:, 0:128]
        msg[width + 32 : width + 48, :] = rows[:, 128:256]
    residual[0:width, :] = jnp.where(columns[width : 2 * width, 1:2] != 0.0, gap_down[...], 0.0)
    residual[width:, :] = jnp.where(columns[3 * width :, 1:2] != 0.0, gap_right[...], 0.0)


def flex_kernel(
    grid, here, link_rows, place, blocks, flex_hbm, pick_flex_hbm, link_flex_hbm, coarse_rows,
    flex, pick_flex, link_flex, arrived,
):
    load = pltpu.make_async_copy(flex_hbm, flex, arrived.at[0])
    load.start()
    row_unknowns, last_window = grid
    count = row_unknowns // 3
    first = row_unknowns * (here[0] - 1)
    offset = first - jnp.clip(first >> 7, 0, last_window) * 128
    row = lax.broadcasted_iota(jnp.int32, (coarse_rows.shape[0], 1), 0)
    j = row >> 4
    part = ((row & 15) * 11) >> 5
    mode = (row & 15) - 3 * part
    down = jnp.where(part == 1, -1, jnp.where(part == 2, 1, 0))
    j = j + jnp.where(part == 3, -1, jnp.where(part == 4, 1, 0))
    valid = (part < 5) & (j >= 0) & (j < count)
    wanted = jnp.where(valid, ((down + 1) * count + j) * 3 + mode + offset, -1)
    at = lax.broadcasted_iota(jnp.int32, (coarse_rows.shape[0], blocks.shape[1]), 1)
    chosen = jnp.where(at == wanted, 1.0, 0.0).astype(BF16)
    high, mid, low = split3(blocks[...])
    coarse_rows[...] = dot_nt(chosen, high) + (dot_nt(chosen, mid) + dot_nt(chosen, low))
    pick_value = picking(jnp.transpose(link_rows[...]))
    load.wait()
    rows = dot(pick_value, flex[...]).astype(BF16)
    pick_flex[...] = rows
    store = pltpu.make_async_copy(pick_flex, pick_flex_hbm, arrived.at[1])
    store.start()
    link_flex[...] = dot(rows, place[...]).astype(BF16)
    store_link = pltpu.make_async_copy(link_flex, link_flex_hbm, arrived.at[2])
    store_link.start()
    store.wait()
    store_link.wait()


def coarse_in_kernel(own, above, below, left, right, mode_rows, precond, coarse):
    width = own.shape[0] // 4
    full = own[...] + jnp.concatenate(
        [above[0:width], below[0:width], left[0:width], right[0:width]], axis=0
    )
    precond[...] = full
    rows = dot_exact(mode_rows[...], full)
    rows = jnp.where(lax.broadcasted_iota(jnp.int32, rows.shape, 0) < 3, rows, 0.0)
    for i in range(coarse.shape[0] // 8):
        coarse[8 * i : 8 * i + 8, :] = rows


def tables_kernel(
    above, below, left, right, mode_rows, link_rows, saved, images, residual, precond, link_flex_hbm,
    mode_six, search_six, forms, sums,
    link_flex, arrived,
):
    load = pltpu.make_async_copy(link_flex_hbm, link_flex, arrived.at[0])
    load.start()
    total = mode_rows.shape[1]
    width = total // 4
    tiles = tile_matrix()
    near = lax.broadcasted_iota(jnp.int32, (1, 256), 1) < width
    used = link_rows[1:2, :] != 0.0
    row = lax.broadcasted_iota(jnp.int32, (16, total), 0)
    mine = jnp.concatenate([mode_rows[...], jnp.zeros((8, total), F32)], axis=0)
    modes = jnp.where(row < 3, mine, 0.0)
    for f, msg in enumerate((above, below, left, right)):
        theirs = jnp.concatenate([msg[width : width + 8], msg[width + 8 : width + 16]], axis=1)
        theirs = at_lanes(widened(jnp.where(near, theirs, 0.0), total), width * f)
        theirs = jnp.concatenate([theirs, jnp.zeros((8, total), F32)], axis=0)
        theirs = jnp.where(row < 3, theirs, 0.0)
        modes = modes + pltpu.roll(theirs, 3 * (1 + f), 0)
    modes = jnp.where(used, modes, 0.0)
    mode_six[...] = six_left(
        lax.dot_general(modes, tiles, (((0,), (0,)), ((), ())), precision=HIGHEST, preferred_element_type=F32)
    )
    search = jnp.zeros((16, total), F32)
    for f in range(4):
        if f % 2 == 0:
            msg = above if f == 0 else left
            piece = jnp.concatenate(
                [msg[width + 16 : width + 32], msg[width + 32 : width + 48]], axis=1
            )
        else:
            piece = lane_window(saved[...], 0 if f == 1 else width, 256)
        search = search + at_lanes(widened(jnp.where(near, piece, 0.0), total), width * f)
    search = jnp.where(used, search, 0.0)
    search_tiled = lax.dot_general(
        search, tiles, (((0,), (0,)), ((), ())), precision=HIGHEST, preferred_element_type=F32
    )
    search_six[...] = six_left(search_tiled)
    lanes = lax.broadcasted_iota(jnp.int32, (16, total), 1)
    image = widened(images[...], total)
    image_down = at_lanes(image, width)
    image_right = at_lanes(image, 2 * width)
    forms[0:16, :] = jnp.where(
        (lanes >= width) & (lanes < 2 * width),
        image_down,
        jnp.where(lanes >= 3 * width, image_right, 0.0),
    )
    energy = jnp.sum(residual[0:width] * precond[width : 2 * width], axis=0, keepdims=True) + jnp.sum(
        residual[width:] * precond[3 * width :], axis=0, keepdims=True
    )
    load.wait()
    flex_search = select_lanes(search, link_flex[...])
    forms[16:32, :] = flex_search
    products = dot_exact(flex_search, search_tiled)
    group = lax.broadcasted_iota(jnp.int32, (16, 128), 1) // 16
    part = lax.broadcasted_iota(jnp.int32, (16, 128), 0)
    products = jnp.where(group == part % 8, products, 0.0)
    sums[...] = jnp.concatenate(
        [
            energy,
            jnp.zeros((1, 128), F32),
            jnp.sum(products[0:8], axis=0, keepdims=True),
            jnp.sum(products[8:16], axis=0, keepdims=True),
            jnp.zeros((4, 128), F32),
        ],
        axis=0,
    )


def coarse_kernel(coarse_rows, gathered, parts):
    parts[...] = dot_exact(coarse_rows[...], gathered[...])


def block_sum(ref, height):
    out = ref[0:height]
    for j in range(1, ref.shape[0] // height):
        out = out + ref[height * j : height * j + height]
    return out


def project_kernel(
    chunk, arrived, precond, mode_six, forms, sums, link_flex_hbm, projected, partial,
    link_flex, copied,
):
    load = pltpu.make_async_copy(link_flex_hbm, link_flex, copied.at[0])
    load.start()
    links = precond[...] - dot(mode_six[...], six_right(block_sum(arrived, 16)))
    projected[...] = links
    linear = dot_exact(forms[...], links)
    high, mid, _ = split3(links)
    parts = jnp.concatenate([high, mid], axis=1)
    load.wait()
    image = dot(link_flex[...], parts)
    square = jnp.sum(links * (image[:, :128] + image[:, 128:]), axis=0, keepdims=True)
    row = lax.broadcasted_iota(jnp.int32, (8, 128), 0)
    last = jnp.where(row == 1, square, sums[...])
    padding = jnp.zeros((partial.shape[0] // 2 - 40, 128), F32)
    full = jnp.concatenate([linear, last, padding], axis=0)
    for j in range(partial.shape[0] // chunk):
        at = chunk * (j // 2)
        partial[chunk * j : chunk * j + chunk, :] = full[at : at + chunk]


def spread_sum_kernel(height, arrived, partial):
    out = block_sum(arrived, height)
    for i in range(partial.shape[0] // height):
        partial[height * i : height * i + height, :] = out


def search_kernel(
    sums, projected, search_six, place, pick_flex_hbm,
    up_msg, left_msg, own, search_own, step,
    pick_flex, arrived,
):
    load = pltpu.make_async_copy(pick_flex_hbm, pick_flex, arrived.at[0])
    load.start()
    width = up_msg.shape[0]
    intersect = sums[0:16]
    cross = sums[16:32]
    energy = sums[32:33]
    square = sums[33:34]
    search = projected[...] - dot(search_six[...], six_right(intersect))
    lifted = select_rows(place[...], search).astype(BF16)
    load.wait()
    image = dot(pick_flex[...], lifted)
    up_msg[...] = image[0:width]
    own[0:width, :] = image[width : 2 * width]
    left_msg[...] = image[2 * width : 3 * width]
    own[width:, :] = image[3 * width :]
    search_own[0:width, :] = search[width : 2 * width]
    search_own[width:, :] = search[3 * width :]
    group = lax.broadcasted_iota(jnp.int32, (16, 128), 1) // 16
    part = lax.broadcasted_iota(jnp.int32, (16, 128), 0)
    packed = jnp.where(part < 8, sums[34:35], sums[35:36])
    packed = jnp.where(group == part % 8, packed, 0.0)
    products = dot_exact(packed, jnp.concatenate([intersect] * 8, axis=0))
    curvature = square + jnp.sum(intersect * (products - 2.0 * cross), axis=0, keepdims=True)
    step[...] = jnp.broadcast_to(energy / curvature, step.shape)


def multiply_kernel(search_own, step, multipliers):
    multipliers[...] = step[0:1] * search_own[...]


def residual_kernel(before, own, below, right, step, residual):
    width = below.shape[0]
    size = step[0:1]
    residual[0:width, :] = before[0:width] - size * (own[0:width] + below[...])
    residual[width:, :] = before[width:] - size * (own[width:] + right[...])


VMEM_LIMIT = 24 * 1024 * 1024
VMEM = pl.BlockSpec(memory_space=pltpu.VMEM)
SMEM = pl.BlockSpec(memory_space=pltpu.SMEM)
HBM = pl.BlockSpec(memory_space=pltpu.HBM)


def call(kernel, inputs, outputs, scalars=0, remote=0, scratch=(), copies=0, hbm_out=(), flops=0):
    out_specs = tuple(HBM if n in hbm_out else VMEM for n in range(len(outputs)))
    outputs = tuple(
        pltpu.HBM(shape, dtype) if n in hbm_out else jax.ShapeDtypeStruct(shape, dtype)
        for n, (shape, dtype) in enumerate(outputs)
    )
    local = len(inputs) - remote
    inputs = tuple(
        x if n < local else pltpu.with_memory_space_constraint(x, pltpu.HBM)
        for n, x in enumerate(inputs)
    )
    scratch = [
        entry if not isinstance(entry, tuple) else pltpu.VMEM(*entry) for entry in scratch
    ]
    if copies:
        scratch.append(pltpu.SemaphoreType.DMA((copies,)))
    return pl.pallas_call(
        kernel,
        out_shape=outputs,
        in_specs=[SMEM] * scalars + [VMEM] * (len(inputs) - scalars - remote) + [HBM] * remote,
        out_specs=out_specs,
        scratch_shapes=scratch,
        cost_estimate=pl.CostEstimate(flops=flops, transcendentals=0, bytes_accessed=0),
        compiler_params=pltpu.CompilerParams(vmem_limit_bytes=VMEM_LIMIT),
    )(*inputs)


def step(
    gap_load, flexibility, schur_blocks, body_modes, coarse_inverse,
    saved_search, saved_images, face_slots, face_count, multiplicity,
):
    rows = lax.axis_size(GX)
    columns = lax.axis_size(GY)
    gap = gap_load[0, 0]
    flex = flexibility[0, 0]
    modes = jnp.transpose(body_modes, (0, 2, 1, 3))[0]
    saved = saved_search[0, 0]
    images = saved_images[0, 0]
    slots = face_slots[0, 0]
    count = face_count[0]
    width = slots.shape[1]
    total = 4 * width
    cases = gap.shape[1]
    unknowns = coarse_inverse.shape[1]
    row_unknowns = columns * modes.shape[0]
    window = min(unknowns, 384)
    windows = [
        min(max((row_unknowns * (i - 1)) // 128, 0), (unknowns - window) // 128) * 128
        for i in range(rows)
    ]
    here = lax.axis_index(GX).reshape(1)
    big = (total, total)
    cube = 2 * total**3
    gap_down, gap_right, blocks = call(
        functools.partial(first_kernel, windows),
        (gap, coarse_inverse),
        (((width, cases), F32), ((width, cases), F32), ((8 * rows, window), F32)),
        remote=2,
        scratch=((coarse_inverse.shape, F32), ((8, unknowns), F32)),
        copies=3,
        flops=cube // 64,
    )
    above = shifted(gap_down, GX, 1)
    left = shifted(gap_right, GY, 1)
    blocks = lax.all_to_all(blocks, GX, 0, 0, tiled=True)
    place, pick_schur, mode_rows, link_rows, slot_cols = call(
        prepare_kernel,
        (count, slots, multiplicity[0], modes, schur_blocks[0, 0]),
        (
            (big, BF16), (big, BF16), ((8, total), F32), ((8, total), F32), ((total, 8), F32),
        ),
        remote=5,
        scratch=(
            ((8, total), F32), (slots.shape, jnp.int32), ((1, total), jnp.int32), (modes.shape, F32),
            (big, BF16), pltpu.SMEM((1, 4), jnp.int32),
        ),
        copies=5,
        flops=cube,
    )
    up_msg, down_msg, left_msg, right_msg, own, residual = call(
        precond_kernel,
        (gap_down, gap_right, above, left, place, pick_schur, slot_cols, mode_rows, saved),
        tuple(((width + extra, cases), F32) for extra in (16, 48, 16, 48))
        + (((total, cases), F32), ((2 * width, cases), F32)),
        flops=cube // 2,
    )
    from_above = shifted(down_msg, GX, 1)
    from_below = shifted(up_msg, GX, -1)
    from_left = shifted(right_msg, GY, 1)
    from_right = shifted(left_msg, GY, -1)
    pick_flex, link_flex, coarse_rows = call(
        functools.partial(flex_kernel, (row_unknowns, (unknowns - window) // 128)),
        (here, link_rows, place, blocks, flex),
        ((big, BF16), (big, BF16), ((16 * columns, 8 * rows), F32)),
        scalars=1,
        remote=1,
        scratch=((big, BF16), (big, BF16), (big, BF16)),
        copies=3,
        hbm_out=(0, 1),
        flops=2 * cube,
    )
    precond, coarse_in = call(
        coarse_in_kernel,
        (own, from_above, from_below, from_left, from_right, mode_rows),
        (((total, cases), F32), ((8 * rows, cases), F32)),
        flops=cube // 16,
    )
    gathered = lax.all_to_all(coarse_in, GX, 0, 0, tiled=True)
    mode_six, search_six, forms, sums = call(
        tables_kernel,
        (
            from_above, from_below, from_left, from_right, mode_rows, link_rows, saved, images,
            residual, precond, link_flex,
        ),
        (((total, 128), BF16), ((total, 128), BF16), ((32, total), F32), ((8, cases), F32)),
        remote=1,
        scratch=((big, BF16),),
        copies=1,
        flops=cube,
    )
    (parts,) = call(
        coarse_kernel, (coarse_rows, gathered), (((16 * columns, cases), F32),), flops=cube // 8,
    )
    parts = lax.all_to_all(parts, GY, 0, 0, tiled=True)
    pairs = columns // 2
    chunk = -(-(-(-40 // pairs)) // 8) * 8
    projected, partial = call(
        functools.partial(project_kernel, chunk),
        (parts, precond, mode_six, forms, sums, link_flex),
        (((total, cases), F32), ((chunk * columns, cases), F32)),
        remote=1,
        scratch=((big, BF16),),
        copies=1,
        flops=cube // 2,
    )
    for axis, following in ((GY, rows), (GX, pairs)):
        partial = lax.all_to_all(partial, axis, 0, 0, tiled=True)
        (partial,) = call(
            functools.partial(spread_sum_kernel, chunk),
            (partial,),
            (((chunk * following, cases), F32),),
            flops=cube // 64,
        )
    sums = lax.all_to_all(partial, GY[0], 0, 0, tiled=True)
    up_msg, left_msg, own, search_own, step = call(
        search_kernel,
        (sums, projected, search_six, place, pick_flex),
        (
            ((width, cases), F32), ((width, cases), F32), ((2 * width, cases), F32),
            ((2 * width, cases), F32), ((8, cases), F32),
        ),
        remote=1,
        scratch=((big, BF16),),
        copies=1,
        flops=cube // 2,
    )
    from_below = shifted(up_msg, GX, -1)
    from_right = shifted(left_msg, GY, -1)
    (multipliers,) = call(
        multiply_kernel, (search_own, step), (((2 * width, cases), F32),), flops=cube // 64,
    )
    (residual,) = call(
        residual_kernel,
        (residual, own, from_below, from_right, step),
        (((2 * width, cases), F32),),
        flops=cube // 64,
    )
    return (multipliers[None, None], residual[None, None])


def split_shape(mesh):
    rows, columns = (mesh.devices.shape[0], mesh.devices.shape[1])
    inner = 4 if rows % 4 == 0 and rows > 4 else 2
    return (rows // inner, inner, columns // 2, 2)


def solution(mesh):
    split = Mesh(mesh.devices.reshape(split_shape(mesh)), GX_GY)
    placed = (
        P(GX, GY, None, None),
        P(GX, GY, None, None),
        P(GX, GY, None, None),
        P(GX, GY, None, None),
        P(GX_GY, None),
        P(GX, GY, None, None),
        P(GX, GY, None, None),
        P(GX, GY, None, None),
        P(GX, GY, None),
        P(GX, GY, None),
    )
    return jax.shard_map(
        step,
        mesh=split,
        in_specs=placed,
        out_specs=(P(GX, GY, None, None), P(GX, GY, None, None)),
        check_vma=False,
    )
```

```python
import functools

import jax
import jax.numpy as jnp
from jax import lax
from jax.experimental import pallas as pl
from jax.experimental.pallas import tpu as pltpu
from jax.sharding import Mesh
from jax.sharding import PartitionSpec as P


GX = ("gx_0", "gx_1")
GY = ("gy_0", "gy_1")
GX_GY = ("gx_0", "gx_1", "gy_0", "gy_1")

F32 = jnp.float32
BF16 = jnp.bfloat16
HIGHEST = lax.Precision.HIGHEST
SIGNS = (-1.0, 1.0, -1.0, 1.0)


def shifted(value, axis, steps):
    count = lax.axis_size(axis)
    initial, last = (max(0, -steps), min(count, count - steps))
    return lax.ppermute(value, axis, [(source, source + steps) for source in range(initial, last)])


def split3(x):
    high = x.astype(BF16)
    rest = x - high.astype(F32)
    mid = rest.astype(BF16)
    low = (rest - mid.astype(F32)).astype(BF16)
    return high, mid, low


def dot(a, b):
    return lax.dot_general(a, b, (((1,), (0,)), ((), ())), preferred_element_type=F32)


def dot_nt(a, b):
    return lax.dot_general(a, b, (((1,), (1,)), ((), ())), preferred_element_type=F32)


def dot_exact(a, b):
    return lax.dot_general(
        a, b, (((1,), (0,)), ((), ())), precision=HIGHEST, preferred_element_type=F32
    )


def dot_exact_nt(a, b):
    return lax.dot_general(
        a, b, (((1,), (1,)), ((), ())), precision=HIGHEST, preferred_element_type=F32
    )


def tiled_columns(rows):
    return lax.dot_general(
        rows, tile_matrix(), (((0,), (0,)), ((), ())), precision=HIGHEST, preferred_element_type=F32
    )


def select_rows(selection, x):
    width = x.shape[1]
    out = dot(selection, jnp.concatenate(split3(x), axis=1))
    return out[:, :width] + (out[:, width : 2 * width] + out[:, 2 * width :])


def select_lanes(x, selection):
    rows = x.shape[0]
    out = dot(jnp.concatenate(split3(x), axis=0), selection)
    return out[:rows] + (out[rows : 2 * rows] + out[2 * rows :])


def six_left(tiled):
    high, mid, low = split3(tiled)
    group = lax.broadcasted_iota(jnp.int32, tiled.shape, 1) // 16
    zero = jnp.zeros_like(tiled)
    is_high = (group == 0) | (group == 1) | (group == 3)
    is_mid = (group == 2) | (group == 4)
    out = jnp.where(
        is_high,
        high.astype(F32),
        jnp.where(is_mid, mid.astype(F32), jnp.where(group == 5, low.astype(F32), zero)),
    )
    return out.astype(BF16)


def six_right(x):
    high, mid, low = split3(x)
    zero = jnp.zeros_like(high)
    return jnp.concatenate([high, mid, high, low, mid, high, zero, zero], axis=0)


def tile_matrix():
    row = lax.broadcasted_iota(jnp.int32, (16, 128), 0)
    lane = lax.broadcasted_iota(jnp.int32, (16, 128), 1)
    return jnp.where(lane % 16 == row, 1.0, 0.0).astype(F32)


def widened(x, lanes):
    return jnp.concatenate([x, jnp.zeros((x.shape[0], lanes - x.shape[1]), x.dtype)], axis=1)


def lane_window(x, start, width):
    total = x.shape[1]
    if start:
        x = pltpu.roll(x, total - start, 1)
    return x[:, :width]


def at_lanes(x, start):
    return pltpu.roll(x, start, 1) if start else x


def prepare_kernel(
    windows, count_hbm, slots_hbm, mult_hbm, modes_hbm, schur_hbm, coarse_hbm,
    place, pick_schur, mode_rows, link_rows, columns, blocks,
    buffer, slots, mult, modes, schur, coarse, wide, count, arrived,
):
    copies = [
        pltpu.make_async_copy(source, target, arrived.at[n])
        for n, (source, target) in enumerate(
            (
                (count_hbm, count), (slots_hbm, slots), (mult_hbm, mult), (modes_hbm, modes),
                (schur_hbm, schur), (coarse_hbm, coarse),
            )
        )
    ]
    for copy in copies:
        copy.start()
    width = slots.shape[1]
    total = 4 * width
    buffer[...] = jnp.zeros_like(buffer)
    wide[...] = jnp.zeros_like(wide)
    lane = lax.broadcasted_iota(jnp.int32, (1, total), 1)
    copies[0].wait()
    copies[1].wait()
    buffer[0:4, 0:width] = slots[...].astype(F32)
    raw = buffer[...]
    slot_row = jnp.zeros((1, total), F32)
    sign_row = jnp.zeros((1, total), F32)
    for f in range(4):
        inside = (lane >= width * f) & (lane < width * f + count[0, f])
        slot_row = jnp.where(inside, at_lanes(raw, width * f)[f : f + 1], slot_row)
        sign_row = jnp.where(inside, SIGNS[f], sign_row)
    copies[2].wait()
    weights = 1.0 / mult[...].astype(F32)
    place_value = placing(slot_row, sign_row)
    place[...] = place_value
    copies[3].wait()
    buffer[...] = jnp.zeros_like(buffer)
    for k in range(modes.shape[0]):
        buffer[k : k + 1, :] = modes[k]
    buffer[3:4, :] = weights
    rows = select_lanes(buffer[...], place_value)
    mode_rows[...] = rows
    buffer[...] = jnp.zeros_like(buffer)
    buffer[0:1, :] = slot_row
    buffer[1:2, :] = sign_row
    buffer[2:3, :] = weights
    buffer[3:4, :] = jnp.abs(rows[3:4])
    link_rows[...] = buffer[...]
    cols = jnp.transpose(buffer[...])
    columns[...] = cols
    pick_value = picking(cols)
    copies[5].wait()
    wide[0:3, :] = coarse[...]
    for i, start in enumerate(windows):
        blocks[8 * i : 8 * i + 8, :] = wide[:, start : start + blocks.shape[1]]
    copies[4].wait()
    pick_schur[...] = dot(pick_value, schur[...]).astype(BF16)


def placing(slot_row, sign_row):
    total = slot_row.shape[1]
    down = lax.broadcasted_iota(jnp.int32, (total, total), 0).astype(F32)
    return jnp.where(down == slot_row, sign_row, 0.0).astype(BF16)


def picking(cols):
    total = cols.shape[0]
    across = lax.broadcasted_iota(jnp.int32, (total, total), 1).astype(F32)
    return jnp.where(across == cols[:, 0:1], cols[:, 1:2], 0.0).astype(BF16)


def precond_kernel(
    gap_down, gap_right, above, left, place, pick_schur, columns, mode_rows, saved,
    up_msg, down_msg, left_msg, right_msg, own, residual,
):
    width = above.shape[0]
    links = jnp.concatenate([above[...], gap_down[...], left[...], gap_right[...]], axis=0)
    spread = select_rows(place[...], links)
    weighted = (columns[:, 2:3] * spread).astype(BF16)
    picked = columns[:, 3:4] * dot(pick_schur[...], weighted)
    own[...] = picked
    for f, msg in enumerate((up_msg, down_msg, left_msg, right_msg)):
        msg[0:width, :] = picked[width * f : width * f + width]
        rows = lane_window(mode_rows[...], width * f, 256)
        msg[width : width + 8, :] = rows[:, 0:128]
        msg[width + 8 : width + 16, :] = rows[:, 128:256]
    for start, msg in ((0, down_msg), (width, right_msg)):
        rows = lane_window(saved[...], start, 256)
        msg[width + 16 : width + 32, :] = rows[:, 0:128]
        msg[width + 32 : width + 48, :] = rows[:, 128:256]
    residual[0:width, :] = jnp.where(columns[width : 2 * width, 1:2] != 0.0, gap_down[...], 0.0)
    residual[width:, :] = jnp.where(columns[3 * width :, 1:2] != 0.0, gap_right[...], 0.0)


def flex_kernel(
    grid, here, link_rows, place, blocks, flex_hbm, pick_flex_hbm, link_flex_hbm, coarse_rows,
    flex, pick_flex, link_flex, arrived,
):
    load = pltpu.make_async_copy(flex_hbm, flex, arrived.at[0])
    load.start()
    row_unknowns, last_window = grid
    count = row_unknowns // 3
    first = row_unknowns * (here[0] - 1)
    offset = first - jnp.clip(first >> 7, 0, last_window) * 128
    row = lax.broadcasted_iota(jnp.int32, (coarse_rows.shape[0], 1), 0)
    j = row >> 4
    part = ((row & 15) * 11) >> 5
    mode = (row & 15) - 3 * part
    down = jnp.where(part == 1, -1, jnp.where(part == 2, 1, 0))
    j = j + jnp.where(part == 3, -1, jnp.where(part == 4, 1, 0))
    valid = (part < 5) & (j >= 0) & (j < count)
    wanted = jnp.where(valid, ((down + 1) * count + j) * 3 + mode + offset, -1)
    at = lax.broadcasted_iota(jnp.int32, (coarse_rows.shape[0], blocks.shape[1]), 1)
    chosen = jnp.where(at == wanted, 1.0, 0.0).astype(BF16)
    high, mid, low = split3(blocks[...])
    coarse_rows[...] = dot_nt(chosen, high) + (dot_nt(chosen, mid) + dot_nt(chosen, low))
    pick_value = picking(jnp.transpose(link_rows[...]))
    load.wait()
    rows = dot(pick_value, flex[...]).astype(BF16)
    pick_flex[...] = rows
    store = pltpu.make_async_copy(pick_flex, pick_flex_hbm, arrived.at[1])
    store.start()
    link_flex[...] = dot(rows, place[...]).astype(BF16)
    store_link = pltpu.make_async_copy(link_flex, link_flex_hbm, arrived.at[2])
    store_link.start()
    store.wait()
    store_link.wait()


def coarse_in_kernel(own, above, below, left, right, mode_rows, precond, coarse):
    width = own.shape[0] // 4
    full = own[...] + jnp.concatenate(
        [above[0:width], below[0:width], left[0:width], right[0:width]], axis=0
    )
    precond[...] = full
    rows = dot_exact(mode_rows[...], full)
    rows = jnp.where(lax.broadcasted_iota(jnp.int32, rows.shape, 0) < 3, rows, 0.0)
    for i in range(coarse.shape[0] // 8):
        coarse[8 * i : 8 * i + 8, :] = rows


def tables_kernel(
    above, below, left, right, mode_rows, link_rows, saved, images, residual, precond, link_flex_hbm,
    mode_six, search_rows, base, mode_forms,
    link_flex, arrived,
):
    load = pltpu.make_async_copy(link_flex_hbm, link_flex, arrived.at[0])
    load.start()
    total = mode_rows.shape[1]
    width = total // 4
    near = lax.broadcasted_iota(jnp.int32, (1, 256), 1) < width
    used = link_rows[1:2, :] != 0.0
    row = lax.broadcasted_iota(jnp.int32, (16, total), 0)
    mine = jnp.concatenate([mode_rows[...], jnp.zeros((8, total), F32)], axis=0)
    modes = jnp.where(row < 3, mine, 0.0)
    for f, msg in enumerate((above, below, left, right)):
        theirs = jnp.concatenate([msg[width : width + 8], msg[width + 8 : width + 16]], axis=1)
        theirs = at_lanes(widened(jnp.where(near, theirs, 0.0), total), width * f)
        theirs = jnp.concatenate([theirs, jnp.zeros((8, total), F32)], axis=0)
        theirs = jnp.where(row < 3, theirs, 0.0)
        modes = modes + pltpu.roll(theirs, 3 * (1 + f), 0)
    modes = jnp.where(used, modes, 0.0)
    modes_tiled = tiled_columns(modes)
    mode_six[...] = six_left(modes_tiled)
    search = jnp.zeros((16, total), F32)
    for f in range(4):
        if f % 2 == 0:
            msg = above if f == 0 else left
            piece = jnp.concatenate(
                [msg[width + 16 : width + 32], msg[width + 32 : width + 48]], axis=1
            )
        else:
            piece = lane_window(saved[...], 0 if f == 1 else width, 256)
        search = search + at_lanes(widened(jnp.where(near, piece, 0.0), total), width * f)
    search = jnp.where(used, search, 0.0)
    search_rows[...] = search
    lanes = lax.broadcasted_iota(jnp.int32, (16, total), 1)
    image = widened(images[...], total)
    image = jnp.where(
        (lanes >= width) & (lanes < 2 * width),
        at_lanes(image, width),
        jnp.where(lanes >= 3 * width, at_lanes(image, 2 * width), 0.0),
    )
    load.wait()
    flexed = select_lanes(jnp.concatenate([search, modes], axis=0), link_flex[...])
    forms = jnp.concatenate([image, flexed], axis=0)
    full = precond[...]
    base[0:48, :] = dot_exact(forms, full)
    mode_forms[...] = six_left(dot_exact(forms, modes_tiled))
    high, mid, _ = split3(full)
    applied = dot(link_flex[...], jnp.concatenate([high, mid], axis=1))
    square = jnp.sum(full * (applied[:, :128] + applied[:, 128:]), axis=0, keepdims=True)
    products = dot_exact(dot_exact_nt(flexed[0:16], search), tile_matrix())
    group = lax.broadcasted_iota(jnp.int32, (16, 128), 1) // 16
    part = lax.broadcasted_iota(jnp.int32, (16, 128), 0)
    products = jnp.where(group == part % 8, products, 0.0)
    energy = jnp.sum(residual[0:width] * full[width : 2 * width], axis=0, keepdims=True) + jnp.sum(
        residual[width:] * full[3 * width :], axis=0, keepdims=True
    )
    base[48:56, :] = jnp.concatenate(
        [
            energy,
            square,
            jnp.sum(products[0:8], axis=0, keepdims=True),
            jnp.sum(products[8:16], axis=0, keepdims=True),
            jnp.zeros((4, 128), F32),
        ],
        axis=0,
    )


def coarse_kernel(coarse_rows, gathered, parts):
    parts[...] = dot_exact(coarse_rows[...], gathered[...])


def block_sum(ref, height):
    out = ref[0:height]
    for j in range(1, ref.shape[0] // height):
        out = out + ref[height * j : height * j + height]
    return out


def project_kernel(chunk, arrived, base, mode_forms, amplitudes, partial):
    y = block_sum(arrived, 16)
    amplitudes[...] = y
    moved = dot(mode_forms[...], six_right(y))
    linear = base[0:32] - moved[0:32]
    square = jnp.sum(y * (moved[32:48] - 2.0 * base[32:48]), axis=0, keepdims=True)
    row = lax.broadcasted_iota(jnp.int32, (8, 128), 0)
    last = base[48:56] + jnp.where(row == 1, square, 0.0)
    padding = jnp.zeros((partial.shape[0] // 2 - 40, 128), F32)
    full = jnp.concatenate([linear, last, padding], axis=0)
    for j in range(partial.shape[0] // chunk):
        at = chunk * (j // 2)
        partial[chunk * j : chunk * j + chunk, :] = full[at : at + chunk]


def own_rows(x, width):
    return jnp.concatenate([x[width : 2 * width], x[3 * width :]], axis=0)


def lift_kernel(
    amplitudes, precond, mode_six, search_rows, link_rows,
    slot_values, slot_six, link_values, link_six,
):
    links = precond[...] - dot(mode_six[...], six_right(amplitudes[...]))
    width = links.shape[0] // 4
    link_values[...] = own_rows(links, width)
    search = search_rows[...]
    link_six[...] = six_left(own_rows(tiled_columns(search), width))
    place = placing(link_rows[0:1], link_rows[1:2])
    slot_values[...] = select_rows(place, links)
    parts = dot_nt(jnp.concatenate(split3(search), axis=0), place)
    slot_six[...] = six_left(tiled_columns(parts[0:16] + (parts[16:32] + parts[32:48])))


def spread_sum_kernel(height, arrived, partial):
    out = block_sum(arrived, height)
    for i in range(partial.shape[0] // height):
        partial[height * i : height * i + height, :] = out


def search_kernel(sums, slot_values, slot_six, pick_flex, up_msg, left_msg, own):
    width = up_msg.shape[0]
    lifted = slot_values[...] - dot(slot_six[...], six_right(sums[0:16]))
    image = dot(pick_flex[...], lifted.astype(BF16))
    up_msg[...] = image[0:width]
    left_msg[...] = image[2 * width : 3 * width]
    own[...] = own_rows(image, width)


def multiply_kernel(sums, link_values, link_six, multipliers, step):
    intersect = sums[0:16]
    cross = sums[16:32]
    energy = sums[32:33]
    square = sums[33:34]
    group = lax.broadcasted_iota(jnp.int32, (16, 128), 1) // 16
    part = lax.broadcasted_iota(jnp.int32, (16, 128), 0)
    packed = jnp.where(part < 8, sums[34:35], sums[35:36])
    packed = jnp.where(group == part % 8, packed, 0.0)
    products = dot_exact(packed, jnp.concatenate([intersect] * 8, axis=0))
    curvature = square + jnp.sum(intersect * (products - 2.0 * cross), axis=0, keepdims=True)
    size = energy / curvature
    step[...] = jnp.broadcast_to(size, step.shape)
    multipliers[...] = size * (link_values[...] - dot(link_six[...], six_right(intersect)))


def residual_kernel(before, own, below, right, step, residual):
    width = below.shape[0]
    size = step[0:1]
    residual[0:width, :] = before[0:width] - size * (own[0:width] + below[...])
    residual[width:, :] = before[width:] - size * (own[width:] + right[...])


VMEM_LIMIT = 24 * 1024 * 1024
VMEM = pl.BlockSpec(memory_space=pltpu.VMEM)
SMEM = pl.BlockSpec(memory_space=pltpu.SMEM)
HBM = pl.BlockSpec(memory_space=pltpu.HBM)


def call(kernel, inputs, outputs, scalars=0, remote=0, scratch=(), copies=0, hbm_out=(), flops=0):
    out_specs = tuple(HBM if n in hbm_out else VMEM for n in range(len(outputs)))
    outputs = tuple(
        pltpu.HBM(shape, dtype) if n in hbm_out else jax.ShapeDtypeStruct(shape, dtype)
        for n, (shape, dtype) in enumerate(outputs)
    )
    local = len(inputs) - remote
    inputs = tuple(
        x if n < local else pltpu.with_memory_space_constraint(x, pltpu.HBM)
        for n, x in enumerate(inputs)
    )
    scratch = [
        entry if not isinstance(entry, tuple) else pltpu.VMEM(*entry) for entry in scratch
    ]
    if copies:
        scratch.append(pltpu.SemaphoreType.DMA((copies,)))
    return pl.pallas_call(
        kernel,
        out_shape=outputs,
        in_specs=[SMEM] * scalars + [VMEM] * (len(inputs) - scalars - remote) + [HBM] * remote,
        out_specs=out_specs,
        scratch_shapes=scratch,
        cost_estimate=pl.CostEstimate(flops=flops, transcendentals=0, bytes_accessed=0),
        compiler_params=pltpu.CompilerParams(vmem_limit_bytes=VMEM_LIMIT),
    )(*inputs)


def step(
    gap_load, flexibility, schur_blocks, body_modes, coarse_inverse,
    saved_search, saved_images, face_slots, face_count, multiplicity,
):
    rows = lax.axis_size(GX)
    columns = lax.axis_size(GY)
    gap = gap_load[0, 0]
    flex = flexibility[0, 0]
    modes = jnp.transpose(body_modes, (0, 2, 1, 3))[0]
    saved = saved_search[0, 0]
    images = saved_images[0, 0]
    slots = face_slots[0, 0]
    count = face_count[0]
    width = slots.shape[1]
    total = 4 * width
    cases = gap.shape[1]
    unknowns = coarse_inverse.shape[1]
    row_unknowns = columns * modes.shape[0]
    window = min(unknowns, 384)
    windows = [
        min(max((row_unknowns * (i - 1)) // 128, 0), (unknowns - window) // 128) * 128
        for i in range(rows)
    ]
    here = lax.axis_index(GX).reshape(1)
    big = (total, total)
    cube = 2 * total**3
    gap_down = gap[:width]
    gap_right = gap[width:]
    above = shifted(gap_down, GX, 1)
    left = shifted(gap_right, GY, 1)
    place, pick_schur, mode_rows, link_rows, slot_cols, blocks = call(
        functools.partial(prepare_kernel, windows),
        (count, slots, multiplicity[0], modes, schur_blocks[0, 0], coarse_inverse),
        (
            (big, BF16), (big, BF16), ((8, total), F32), ((8, total), F32), ((total, 8), F32),
            ((8 * rows, window), F32),
        ),
        remote=6,
        scratch=(
            ((8, total), F32), (slots.shape, jnp.int32), ((1, total), jnp.int32), (modes.shape, F32),
            (big, BF16), (coarse_inverse.shape, F32), ((8, unknowns), F32),
            pltpu.SMEM((1, 4), jnp.int32),
        ),
        copies=6,
        flops=cube,
    )
    up_msg, down_msg, left_msg, right_msg, own, residual = call(
        precond_kernel,
        (gap_down, gap_right, above, left, place, pick_schur, slot_cols, mode_rows, saved),
        tuple(((width + extra, cases), F32) for extra in (16, 48, 16, 48))
        + (((total, cases), F32), ((2 * width, cases), F32)),
        flops=cube // 2,
    )
    from_above = shifted(down_msg, GX, 1)
    from_below = shifted(up_msg, GX, -1)
    from_left = shifted(right_msg, GY, 1)
    from_right = shifted(left_msg, GY, -1)
    blocks = lax.all_to_all(blocks, GX, 0, 0, tiled=True)
    precond, coarse_in = call(
        coarse_in_kernel,
        (own, from_above, from_below, from_left, from_right, mode_rows),
        (((total, cases), F32), ((8 * rows, cases), F32)),
        flops=cube // 16,
    )
    gathered = lax.all_to_all(coarse_in, GX, 0, 0, tiled=True)
    pick_flex, link_flex, coarse_rows = call(
        functools.partial(flex_kernel, (row_unknowns, (unknowns - window) // 128)),
        (here, link_rows, place, blocks, flex),
        ((big, BF16), (big, BF16), ((16 * columns, 8 * rows), F32)),
        scalars=1,
        remote=1,
        scratch=((big, BF16), (big, BF16), (big, BF16)),
        copies=3,
        hbm_out=(0, 1),
        flops=2 * cube,
    )
    (parts,) = call(
        coarse_kernel, (coarse_rows, gathered), (((16 * columns, cases), F32),), flops=cube // 8,
    )
    parts = lax.all_to_all(parts, GY, 0, 0, tiled=True)
    mode_six, search_rows, base, mode_forms = call(
        tables_kernel,
        (
            from_above, from_below, from_left, from_right, mode_rows, link_rows, saved, images,
            residual, precond, link_flex,
        ),
        (((total, 128), BF16), ((16, total), F32), ((56, cases), F32), ((48, 128), BF16)),
        remote=1,
        scratch=((big, BF16),),
        copies=1,
        flops=cube,
    )
    pairs = columns // 2
    chunk = -(-(-(-40 // pairs)) // 8) * 8
    amplitudes, partial = call(
        functools.partial(project_kernel, chunk),
        (parts, base, mode_forms),
        (((16, cases), F32), ((chunk * columns, cases), F32)),
        flops=cube // 64,
    )
    slot_values, slot_six, link_values, link_six = call(
        lift_kernel,
        (amplitudes, precond, mode_six, search_rows, link_rows),
        (
            ((total, cases), F32), ((total, 128), BF16), ((2 * width, cases), F32),
            ((2 * width, 128), BF16),
        ),
        flops=cube,
    )
    for axis, following in ((GY, rows), (GX, pairs)):
        partial = lax.all_to_all(partial, axis, 0, 0, tiled=True)
        (partial,) = call(
            functools.partial(spread_sum_kernel, chunk),
            (partial,),
            (((chunk * following, cases), F32),),
            flops=cube // 64,
        )
    sums = lax.all_to_all(partial, GY[0], 0, 0, tiled=True)
    up_msg, left_msg, own = call(
        search_kernel,
        (sums, slot_values, slot_six, pick_flex),
        (((width, cases), F32), ((width, cases), F32), ((2 * width, cases), F32)),
        flops=cube // 2,
    )
    from_below = shifted(up_msg, GX, -1)
    from_right = shifted(left_msg, GY, -1)
    multipliers, step = call(
        multiply_kernel,
        (sums, link_values, link_six),
        (((2 * width, cases), F32), ((8, cases), F32)),
        flops=cube // 64,
    )
    (residual,) = call(
        residual_kernel,
        (residual, own, from_below, from_right, step),
        (((2 * width, cases), F32),),
        flops=cube // 64,
    )
    return (multipliers[None, None], residual[None, None])


def split_shape(mesh):
    rows, columns = (mesh.devices.shape[0], mesh.devices.shape[1])
    inner = 4 if rows % 4 == 0 and rows > 4 else 2
    return (rows // inner, inner, columns // 2, 2)


def solution(mesh):
    split = Mesh(mesh.devices.reshape(split_shape(mesh)), GX_GY)
    placed = (
        P(GX, GY, None, None),
        P(GX, GY, None, None),
        P(GX, GY, None, None),
        P(GX, GY, None, None),
        P(GX_GY, None),
        P(GX, GY, None, None),
        P(GX, GY, None, None),
        P(GX, GY, None, None),
        P(GX, GY, None),
        P(GX, GY, None),
    )
    return jax.shard_map(
        step,
        mesh=split,
        in_specs=placed,
        out_specs=(P(GX, GY, None, None), P(GX, GY, None, None)),
        check_vma=False,
    )
```

```python
import functools

import jax
import jax.numpy as jnp
from jax import lax
from jax.experimental import pallas as pl
from jax.experimental.pallas import tpu as pltpu
from jax.sharding import Mesh
from jax.sharding import PartitionSpec as P


GX = ("gx_0", "gx_1")
GY = ("gy_0", "gy_1")
GX_GY = ("gx_0", "gx_1", "gy_0", "gy_1")

F32 = jnp.float32
BF16 = jnp.bfloat16
HIGHEST = lax.Precision.HIGHEST
SIGNS = (-1.0, 1.0, -1.0, 1.0)


def shifted(value, axis, steps):
    count = lax.axis_size(axis)
    initial, last = (max(0, -steps), min(count, count - steps))
    return lax.ppermute(value, axis, [(source, source + steps) for source in range(initial, last)])


def split3(x):
    high = x.astype(BF16)
    rest = x - high.astype(F32)
    mid = rest.astype(BF16)
    low = (rest - mid.astype(F32)).astype(BF16)
    return high, mid, low


def dot(a, b):
    return lax.dot_general(a, b, (((1,), (0,)), ((), ())), preferred_element_type=F32)


def dot_nt(a, b):
    return lax.dot_general(a, b, (((1,), (1,)), ((), ())), preferred_element_type=F32)


def dot_exact(a, b):
    return lax.dot_general(
        a, b, (((1,), (0,)), ((), ())), precision=HIGHEST, preferred_element_type=F32
    )


def dot_exact_nt(a, b):
    return lax.dot_general(
        a, b, (((1,), (1,)), ((), ())), precision=HIGHEST, preferred_element_type=F32
    )


def tiled_columns(rows):
    return lax.dot_general(
        rows, tile_matrix(), (((0,), (0,)), ((), ())), precision=HIGHEST, preferred_element_type=F32
    )


def select_rows(selection, x):
    width = x.shape[1]
    out = dot(selection, jnp.concatenate(split3(x), axis=1))
    return out[:, :width] + (out[:, width : 2 * width] + out[:, 2 * width :])


def select_lanes(x, selection):
    rows = x.shape[0]
    out = dot(jnp.concatenate(split3(x), axis=0), selection)
    return out[:rows] + (out[rows : 2 * rows] + out[2 * rows :])


def six_left(tiled):
    high, mid, low = split3(tiled)
    group = lax.broadcasted_iota(jnp.int32, tiled.shape, 1) // 16
    zero = jnp.zeros_like(tiled)
    is_high = (group == 0) | (group == 1) | (group == 3)
    is_mid = (group == 2) | (group == 4)
    out = jnp.where(
        is_high,
        high.astype(F32),
        jnp.where(is_mid, mid.astype(F32), jnp.where(group == 5, low.astype(F32), zero)),
    )
    return out.astype(BF16)


def six_right(x):
    high, mid, low = split3(x)
    zero = jnp.zeros_like(high)
    return jnp.concatenate([high, mid, high, low, mid, high, zero, zero], axis=0)


def tile_matrix():
    row = lax.broadcasted_iota(jnp.int32, (16, 128), 0)
    lane = lax.broadcasted_iota(jnp.int32, (16, 128), 1)
    return jnp.where(lane % 16 == row, 1.0, 0.0).astype(F32)


def widened(x, lanes):
    return jnp.concatenate([x, jnp.zeros((x.shape[0], lanes - x.shape[1]), x.dtype)], axis=1)


def lane_window(x, start, width):
    total = x.shape[1]
    if start:
        x = pltpu.roll(x, total - start, 1)
    return x[:, :width]


def at_lanes(x, start):
    return pltpu.roll(x, start, 1) if start else x


def blocks_kernel(coarse_hbm, blocks, coarse, wide, arrived):
    load = pltpu.make_async_copy(coarse_hbm, coarse, arrived.at[0])
    load.start()
    wide[...] = jnp.zeros_like(wide)
    load.wait()
    wide[0:3, :] = coarse[...]
    unknowns = wide.shape[1]
    grid_rows = blocks.shape[0] // 8
    row_unknowns = unknowns // grid_rows
    for i in range(grid_rows):
        first = row_unknowns * (i - 1)
        span = min(unknowns, 384)
        start = min(max(first // 128, 0) * 128, unknowns - span)
        piece = wide[:, start : start + span]
        if first != start:
            piece = pltpu.roll(piece, (start - first) % span, 1)
        if span < 256:
            piece = widened(piece, 256)
        blocks[8 * i : 8 * i + 8, :] = piece[:, 0:128] + pltpu.roll(piece[:, 128:256], 3, 0)


def prepare_kernel(
    count_hbm, slots_hbm, mult_hbm, modes_hbm, schur_hbm,
    place, pick_schur, mode_rows, link_rows,
    buffer, slots, mult, modes, schur, count, arrived,
):
    copies = [
        pltpu.make_async_copy(source, target, arrived.at[n])
        for n, (source, target) in enumerate(
            (
                (count_hbm, count), (slots_hbm, slots), (mult_hbm, mult), (modes_hbm, modes),
                (schur_hbm, schur),
            )
        )
    ]
    for copy in copies:
        copy.start()
    width = slots.shape[1]
    total = 4 * width
    buffer[...] = jnp.zeros_like(buffer)
    lane = lax.broadcasted_iota(jnp.int32, (1, total), 1)
    copies[0].wait()
    copies[1].wait()
    buffer[0:4, 0:width] = slots[...].astype(F32)
    raw = buffer[...]
    slot_row = jnp.zeros((1, total), F32)
    sign_row = jnp.zeros((1, total), F32)
    for f in range(4):
        inside = (lane >= width * f) & (lane < width * f + count[0, f])
        slot_row = jnp.where(inside, at_lanes(raw, width * f)[f : f + 1], slot_row)
        sign_row = jnp.where(inside, SIGNS[f], sign_row)
    copies[2].wait()
    weights = 1.0 / mult[...].astype(F32)
    place_value = placing(slot_row, sign_row)
    place[...] = place_value
    copies[3].wait()
    buffer[...] = jnp.zeros_like(buffer)
    for k in range(modes.shape[0]):
        buffer[k : k + 1, :] = modes[k]
    buffer[3:4, :] = weights
    rows = select_lanes(buffer[...], place_value)
    mode_rows[...] = rows
    buffer[...] = jnp.zeros_like(buffer)
    buffer[0:1, :] = slot_row
    buffer[1:2, :] = sign_row
    buffer[2:3, :] = weights
    buffer[3:4, :] = jnp.abs(rows[3:4])
    link_rows[...] = buffer[...]
    pick_value = picking(jnp.transpose(buffer[...]))
    copies[4].wait()
    pick_schur[...] = dot(pick_value, schur[...]).astype(BF16)


def placing(slot_row, sign_row):
    total = slot_row.shape[1]
    down = lax.broadcasted_iota(jnp.int32, (total, total), 0).astype(F32)
    return jnp.where(down == slot_row, sign_row, 0.0).astype(BF16)


def picking(cols):
    total = cols.shape[0]
    across = lax.broadcasted_iota(jnp.int32, (total, total), 1).astype(F32)
    return jnp.where(across == cols[:, 0:1], cols[:, 1:2], 0.0).astype(BF16)


def precond_kernel(
    gap_down, gap_right, above, left, place, pick_schur, link_rows, mode_rows, saved,
    up_msg, down_msg, left_msg, right_msg, own, residual,
):
    width = above.shape[0]
    columns = jnp.transpose(link_rows[...])
    links = jnp.concatenate([above[...], gap_down[...], left[...], gap_right[...]], axis=0)
    spread = select_rows(place[...], links)
    weighted = (columns[:, 2:3] * spread).astype(BF16)
    picked = columns[:, 3:4] * dot(pick_schur[...], weighted)
    own[...] = picked
    for f, msg in enumerate((up_msg, down_msg, left_msg, right_msg)):
        msg[0:width, :] = picked[width * f : width * f + width]
        rows = lane_window(mode_rows[...], width * f, 256)
        msg[width : width + 8, :] = rows[:, 0:128]
        msg[width + 8 : width + 16, :] = rows[:, 128:256]
    for start, msg in ((0, down_msg), (width, right_msg)):
        rows = lane_window(saved[...], start, 256)
        msg[width + 16 : width + 32, :] = rows[:, 0:128]
        msg[width + 32 : width + 48, :] = rows[:, 128:256]
    residual[0:width, :] = jnp.where(columns[width : 2 * width, 1:2] != 0.0, gap_down[...], 0.0)
    residual[width:, :] = jnp.where(columns[3 * width :, 1:2] != 0.0, gap_right[...], 0.0)


def rows_kernel(blocks, coarse_rows):
    total = coarse_rows.shape[0]
    count = total // 16
    row = lax.broadcasted_iota(jnp.int32, (total, 1), 0)
    j = row >> 4
    part = ((row & 15) * 11) >> 5
    mode = (row & 15) - 3 * part
    down = jnp.where(part == 1, -1, jnp.where(part == 2, 1, 0))
    j = j + jnp.where(part == 3, -1, jnp.where(part == 4, 1, 0))
    valid = (part < 5) & (j >= 0) & (j < count)
    wanted = jnp.where(valid, ((down + 1) * count + j) * 3 + mode, -1)
    at = lax.broadcasted_iota(jnp.int32, (total, 128), 1)
    chosen = [
        jnp.where(at + shift == wanted, 1.0, 0.0).astype(BF16) for shift in (0, 128)
    ]
    chosen = jnp.concatenate(chosen, axis=0)
    high, mid, low = split3(blocks[...])
    out = dot_nt(chosen, high) + (dot_nt(chosen, mid) + dot_nt(chosen, low))
    width = coarse_rows.shape[1]
    coarse_rows[...] = out[:total] + pltpu.roll(out[total:], width - 3, 1)


def flex_kernel(
    link_rows, place, flex_hbm, pick_flex_hbm, link_flex_hbm,
    flex, pick_flex, link_flex, arrived,
):
    load = pltpu.make_async_copy(flex_hbm, flex, arrived.at[0])
    load.start()
    pick_value = picking(jnp.transpose(link_rows[...]))
    load.wait()
    rows = dot(pick_value, flex[...]).astype(BF16)
    pick_flex[...] = rows
    store = pltpu.make_async_copy(pick_flex, pick_flex_hbm, arrived.at[1])
    store.start()
    link_flex[...] = dot(rows, place[...]).astype(BF16)
    store_link = pltpu.make_async_copy(link_flex, link_flex_hbm, arrived.at[2])
    store_link.start()
    store.wait()
    store_link.wait()


def coarse_in_kernel(own, above, below, left, right, mode_rows, precond, coarse):
    width = own.shape[0] // 4
    full = own[...] + jnp.concatenate(
        [above[0:width], below[0:width], left[0:width], right[0:width]], axis=0
    )
    precond[...] = full
    rows = dot_exact(mode_rows[...], full)
    rows = jnp.where(lax.broadcasted_iota(jnp.int32, rows.shape, 0) < 3, rows, 0.0)
    for i in range(coarse.shape[0] // 8):
        coarse[8 * i : 8 * i + 8, :] = rows


def tables_kernel(
    above, below, left, right, mode_rows, link_rows, saved, images, residual, precond, link_flex_hbm,
    mode_six, search_rows, base, mode_forms,
    link_flex, arrived,
):
    load = pltpu.make_async_copy(link_flex_hbm, link_flex, arrived.at[0])
    load.start()
    total = mode_rows.shape[1]
    width = total // 4
    near = lax.broadcasted_iota(jnp.int32, (1, 256), 1) < width
    used = link_rows[1:2, :] != 0.0
    row = lax.broadcasted_iota(jnp.int32, (16, total), 0)
    mine = jnp.concatenate([mode_rows[...], jnp.zeros((8, total), F32)], axis=0)
    modes = jnp.where(row < 3, mine, 0.0)
    for f, msg in enumerate((above, below, left, right)):
        theirs = jnp.concatenate([msg[width : width + 8], msg[width + 8 : width + 16]], axis=1)
        theirs = at_lanes(widened(jnp.where(near, theirs, 0.0), total), width * f)
        theirs = jnp.concatenate([theirs, jnp.zeros((8, total), F32)], axis=0)
        theirs = jnp.where(row < 3, theirs, 0.0)
        modes = modes + pltpu.roll(theirs, 3 * (1 + f), 0)
    modes = jnp.where(used, modes, 0.0)
    modes_tiled = tiled_columns(modes)
    mode_six[...] = six_left(modes_tiled)
    search = jnp.zeros((16, total), F32)
    for f in range(4):
        if f % 2 == 0:
            msg = above if f == 0 else left
            piece = jnp.concatenate(
                [msg[width + 16 : width + 32], msg[width + 32 : width + 48]], axis=1
            )
        else:
            piece = lane_window(saved[...], 0 if f == 1 else width, 256)
        search = search + at_lanes(widened(jnp.where(near, piece, 0.0), total), width * f)
    search = jnp.where(used, search, 0.0)
    search_rows[...] = search
    lanes = lax.broadcasted_iota(jnp.int32, (16, total), 1)
    image = widened(images[...], total)
    image = jnp.where(
        (lanes >= width) & (lanes < 2 * width),
        at_lanes(image, width),
        jnp.where(lanes >= 3 * width, at_lanes(image, 2 * width), 0.0),
    )
    load.wait()
    flexed = select_lanes(jnp.concatenate([search, modes], axis=0), link_flex[...])
    forms = jnp.concatenate([image, flexed], axis=0)
    full = precond[...]
    base[0:48, :] = dot_exact(forms, full)
    mode_forms[...] = six_left(dot_exact(forms, modes_tiled))
    high, mid, _ = split3(full)
    applied = dot(link_flex[...], jnp.concatenate([high, mid], axis=1))
    square = jnp.sum(full * (applied[:, :128] + applied[:, 128:]), axis=0, keepdims=True)
    products = dot_exact(dot_exact_nt(flexed[0:16], search), tile_matrix())
    group = lax.broadcasted_iota(jnp.int32, (16, 128), 1) // 16
    part = lax.broadcasted_iota(jnp.int32, (16, 128), 0)
    products = jnp.where(group == part % 8, products, 0.0)
    energy = jnp.sum(residual[0:width] * full[width : 2 * width], axis=0, keepdims=True) + jnp.sum(
        residual[width:] * full[3 * width :], axis=0, keepdims=True
    )
    base[48:56, :] = jnp.concatenate(
        [
            energy,
            square,
            jnp.sum(products[0:8], axis=0, keepdims=True),
            jnp.sum(products[8:16], axis=0, keepdims=True),
            jnp.zeros((4, 128), F32),
        ],
        axis=0,
    )


def coarse_kernel(coarse_rows, gathered, parts):
    parts[...] = dot_exact(coarse_rows[...], gathered[...])


def block_sum(ref, height):
    out = ref[0:height]
    for j in range(1, ref.shape[0] // height):
        out = out + ref[height * j : height * j + height]
    return out


def project_kernel(chunk, arrived, base, mode_forms, amplitudes, partial):
    y = block_sum(arrived, 16)
    amplitudes[...] = y
    moved = dot(mode_forms[...], six_right(y))
    linear = base[0:32] - moved[0:32]
    square = jnp.sum(y * (moved[32:48] - 2.0 * base[32:48]), axis=0, keepdims=True)
    row = lax.broadcasted_iota(jnp.int32, (8, 128), 0)
    last = base[48:56] + jnp.where(row == 1, square, 0.0)
    padding = jnp.zeros((partial.shape[0] // 2 - 40, 128), F32)
    full = jnp.concatenate([linear, last, padding], axis=0)
    for j in range(partial.shape[0] // chunk):
        at = chunk * (j // 2)
        partial[chunk * j : chunk * j + chunk, :] = full[at : at + chunk]


def own_rows(x, width):
    return jnp.concatenate([x[width : 2 * width], x[3 * width :]], axis=0)


def lift_kernel(
    amplitudes, precond, mode_six, search_rows, link_rows,
    slot_values, slot_six, link_values, link_six,
):
    links = precond[...] - dot(mode_six[...], six_right(amplitudes[...]))
    width = links.shape[0] // 4
    link_values[...] = own_rows(links, width)
    search = search_rows[...]
    link_six[...] = six_left(own_rows(tiled_columns(search), width))
    place = placing(link_rows[0:1], link_rows[1:2])
    slot_values[...] = select_rows(place, links)
    parts = dot_nt(jnp.concatenate(split3(search), axis=0), place)
    slot_six[...] = six_left(tiled_columns(parts[0:16] + (parts[16:32] + parts[32:48])))


def spread_sum_kernel(height, arrived, partial):
    out = block_sum(arrived, height)
    for i in range(partial.shape[0] // height):
        partial[height * i : height * i + height, :] = out


def search_kernel(sums, slot_values, slot_six, pick_flex, up_msg, left_msg, own):
    width = up_msg.shape[0]
    lifted = slot_values[...] - dot(slot_six[...], six_right(sums[0:16]))
    image = dot(pick_flex[...], lifted.astype(BF16))
    up_msg[...] = image[0:width]
    left_msg[...] = image[2 * width : 3 * width]
    own[...] = own_rows(image, width)


def multiply_kernel(sums, link_values, link_six, multipliers, step):
    intersect = sums[0:16]
    cross = sums[16:32]
    energy = sums[32:33]
    square = sums[33:34]
    group = lax.broadcasted_iota(jnp.int32, (16, 128), 1) // 16
    part = lax.broadcasted_iota(jnp.int32, (16, 128), 0)
    packed = jnp.where(part < 8, sums[34:35], sums[35:36])
    packed = jnp.where(group == part % 8, packed, 0.0)
    products = dot_exact(packed, jnp.concatenate([intersect] * 8, axis=0))
    curvature = square + jnp.sum(intersect * (products - 2.0 * cross), axis=0, keepdims=True)
    size = energy / curvature
    step[...] = jnp.broadcast_to(size, step.shape)
    multipliers[...] = size * (link_values[...] - dot(link_six[...], six_right(intersect)))


def residual_kernel(before, own, below, right, step, residual):
    width = below.shape[0]
    size = step[0:1]
    residual[0:width, :] = before[0:width] - size * (own[0:width] + below[...])
    residual[width:, :] = before[width:] - size * (own[width:] + right[...])


VMEM_LIMIT = 24 * 1024 * 1024
VMEM = pl.BlockSpec(memory_space=pltpu.VMEM)
SMEM = pl.BlockSpec(memory_space=pltpu.SMEM)
HBM = pl.BlockSpec(memory_space=pltpu.HBM)


def call(kernel, inputs, outputs, scalars=0, remote=0, scratch=(), copies=0, hbm_out=(), flops=0):
    out_specs = tuple(HBM if n in hbm_out else VMEM for n in range(len(outputs)))
    outputs = tuple(
        pltpu.HBM(shape, dtype)
        if n in hbm_out
        else jax.ShapeDtypeStruct(shape, dtype)
        for n, (shape, dtype) in enumerate(outputs)
    )
    local = len(inputs) - remote
    inputs = tuple(
        x if n < local else pltpu.with_memory_space_constraint(x, pltpu.HBM)
        for n, x in enumerate(inputs)
    )
    scratch = [
        entry if not isinstance(entry, tuple) else pltpu.VMEM(*entry) for entry in scratch
    ]
    if copies:
        scratch.append(pltpu.SemaphoreType.DMA((copies,)))
    return pl.pallas_call(
        kernel,
        out_shape=outputs,
        in_specs=[SMEM] * scalars + [VMEM] * (len(inputs) - scalars - remote) + [HBM] * remote,
        out_specs=out_specs,
        scratch_shapes=scratch,
        cost_estimate=pl.CostEstimate(flops=flops, transcendentals=0, bytes_accessed=0),
        compiler_params=pltpu.CompilerParams(vmem_limit_bytes=VMEM_LIMIT),
    )(*inputs)


def step(
    gap_load, flexibility, schur_blocks, body_modes, coarse_inverse,
    saved_search, saved_images, face_slots, face_count, multiplicity,
):
    rows = lax.axis_size(GX)
    columns = lax.axis_size(GY)
    gap = gap_load[0, 0]
    flex = flexibility[0, 0]
    modes = jnp.transpose(body_modes, (0, 2, 1, 3))[0]
    saved = saved_search[0, 0]
    images = saved_images[0, 0]
    slots = face_slots[0, 0]
    count = face_count[0]
    width = slots.shape[1]
    total = 4 * width
    cases = gap.shape[1]
    unknowns = coarse_inverse.shape[1]
    big = (total, total)
    cube = 2 * total**3
    gap_down = gap[:width]
    gap_right = gap[width:]
    above = shifted(gap_down, GX, 1)
    left = shifted(gap_right, GY, 1)
    (blocks,) = call(
        blocks_kernel,
        (coarse_inverse,),
        (((8 * rows, 128), F32),),
        remote=1,
        scratch=((coarse_inverse.shape, F32), ((8, unknowns), F32)),
        copies=1,
        flops=cube // 64,
    )
    blocks = lax.all_to_all(blocks, GX, 0, 0, tiled=True)
    place, pick_schur, mode_rows, link_rows = call(
        prepare_kernel,
        (count, slots, multiplicity[0], modes, schur_blocks[0, 0]),
        (
            (big, BF16), (big, BF16), ((8, total), F32), ((8, total), F32),
        ),
        remote=5,
        scratch=(
            ((8, total), F32), (slots.shape, jnp.int32), ((1, total), jnp.int32), (modes.shape, F32),
            (big, BF16), pltpu.SMEM((1, 4), jnp.int32),
        ),
        copies=5,
        flops=cube,
    )
    up_msg, down_msg, left_msg, right_msg, own, residual = call(
        precond_kernel,
        (gap_down, gap_right, above, left, place, pick_schur, link_rows, mode_rows, saved),
        tuple(((width + extra, cases), F32) for extra in (16, 48, 16, 48))
        + (((total, cases), F32), ((2 * width, cases), F32)),
        flops=cube // 2,
    )
    from_above = shifted(down_msg, GX, 1)
    from_below = shifted(up_msg, GX, -1)
    from_left = shifted(right_msg, GY, 1)
    from_right = shifted(left_msg, GY, -1)
    precond, coarse_in = call(
        coarse_in_kernel,
        (own, from_above, from_below, from_left, from_right, mode_rows),
        (((total, cases), F32), ((8 * rows, cases), F32)),
        flops=cube // 16,
    )
    gathered = lax.all_to_all(coarse_in, GX, 0, 0, tiled=True)
    pick_flex, link_flex = call(
        flex_kernel,
        (link_rows, place, flex),
        ((big, BF16), (big, BF16)),
        remote=1,
        scratch=((big, BF16), (big, BF16), (big, BF16)),
        copies=3,
        hbm_out=(0, 1),
        flops=2 * cube,
    )
    (coarse_rows,) = call(
        rows_kernel, (blocks,), (((16 * columns, 8 * rows), F32),), flops=cube // 16
    )
    (parts,) = call(
        coarse_kernel, (coarse_rows, gathered), (((16 * columns, cases), F32),), flops=cube // 8,
    )
    parts = lax.all_to_all(parts, GY, 0, 0, tiled=True)
    mode_six, search_rows, base, mode_forms = call(
        tables_kernel,
        (
            from_above, from_below, from_left, from_right, mode_rows, link_rows, saved, images,
            residual, precond, link_flex,
        ),
        (((total, 128), BF16), ((16, total), F32), ((56, cases), F32), ((48, 128), BF16)),
        remote=1,
        scratch=((big, BF16),),
        copies=1,
        flops=cube,
    )
    pairs = columns // 2
    chunk = -(-(-(-40 // pairs)) // 8) * 8
    amplitudes, partial = call(
        functools.partial(project_kernel, chunk),
        (parts, base, mode_forms),
        (((16, cases), F32), ((chunk * columns, cases), F32)),
        flops=cube // 64,
    )
    slot_values, slot_six, link_values, link_six = call(
        lift_kernel,
        (amplitudes, precond, mode_six, search_rows, link_rows),
        (
            ((total, cases), F32), ((total, 128), BF16), ((2 * width, cases), F32),
            ((2 * width, 128), BF16),
        ),
        flops=cube,
    )
    for axis, following in ((GY, rows), (GX, pairs)):
        partial = lax.all_to_all(partial, axis, 0, 0, tiled=True)
        (partial,) = call(
            functools.partial(spread_sum_kernel, chunk),
            (partial,),
            (((chunk * following, cases), F32),),
            flops=cube // 64,
        )
    sums = lax.all_to_all(partial, GY[0], 0, 0, tiled=True)
    up_msg, left_msg, own = call(
        search_kernel,
        (sums, slot_values, slot_six, pick_flex),
        (((width, cases), F32), ((width, cases), F32), ((2 * width, cases), F32)),
        flops=cube // 2,
    )
    from_below = shifted(up_msg, GX, -1)
    from_right = shifted(left_msg, GY, -1)
    multipliers, step = call(
        multiply_kernel,
        (sums, link_values, link_six),
        (((2 * width, cases), F32), ((8, cases), F32)),
        flops=cube // 64,
    )
    (residual,) = call(
        residual_kernel,
        (residual, own, from_below, from_right, step),
        (((2 * width, cases), F32),),
        flops=cube // 64,
    )
    return (multipliers[None, None], residual[None, None])


def split_shape(mesh):
    rows, columns = (mesh.devices.shape[0], mesh.devices.shape[1])
    inner = 4 if rows % 4 == 0 and rows > 4 else 2
    return (rows // inner, inner, columns // 2, 2)


def solution(mesh):
    split = Mesh(mesh.devices.reshape(split_shape(mesh)), GX_GY)
    placed = (
        P(GX, GY, None, None),
        P(GX, GY, None, None),
        P(GX, GY, None, None),
        P(GX, GY, None, None),
        P(GX_GY, None),
        P(GX, GY, None, None),
        P(GX, GY, None, None),
        P(GX, GY, None, None),
        P(GX, GY, None),
        P(GX, GY, None),
    )
    return jax.shard_map(
        step,
        mesh=split,
        in_specs=placed,
        out_specs=(P(GX, GY, None, None), P(GX, GY, None, None)),
        check_vma=False,
    )
```

```python
import functools

import jax
import jax.numpy as jnp
from jax import lax
from jax.experimental import pallas as pl
from jax.experimental.pallas import tpu as pltpu
from jax.sharding import Mesh
from jax.sharding import PartitionSpec as P


GX = ("gx_0", "gx_1")
GY = ("gy_0", "gy_1")
GX_GY = ("gx_0", "gx_1", "gy_0", "gy_1")

F32 = jnp.float32
BF16 = jnp.bfloat16
HIGHEST = lax.Precision.HIGHEST
SIGNS = (-1.0, 1.0, -1.0, 1.0)


def shifted(value, axis, steps):
    count = lax.axis_size(axis)
    initial, last = (max(0, -steps), min(count, count - steps))
    return lax.ppermute(value, axis, [(source, source + steps) for source in range(initial, last)])


def split3(x):
    high = x.astype(BF16)
    rest = x - high.astype(F32)
    mid = rest.astype(BF16)
    low = (rest - mid.astype(F32)).astype(BF16)
    return high, mid, low


def dot(a, b):
    return lax.dot_general(a, b, (((1,), (0,)), ((), ())), preferred_element_type=F32)


def dot_nt(a, b):
    return lax.dot_general(a, b, (((1,), (1,)), ((), ())), preferred_element_type=F32)


def dot_exact(a, b):
    return lax.dot_general(
        a, b, (((1,), (0,)), ((), ())), precision=HIGHEST, preferred_element_type=F32
    )


def dot_exact_nt(a, b):
    return lax.dot_general(
        a, b, (((1,), (1,)), ((), ())), precision=HIGHEST, preferred_element_type=F32
    )


def tiled_columns(rows):
    return lax.dot_general(
        rows, tile_matrix(), (((0,), (0,)), ((), ())), precision=HIGHEST, preferred_element_type=F32
    )


def select_rows(selection, x):
    width = x.shape[1]
    out = dot(selection, jnp.concatenate(split3(x), axis=1))
    return out[:, :width] + (out[:, width : 2 * width] + out[:, 2 * width :])


def select_lanes(x, selection):
    rows = x.shape[0]
    out = dot(jnp.concatenate(split3(x), axis=0), selection)
    return out[:rows] + (out[rows : 2 * rows] + out[2 * rows :])


def six_left(tiled):
    high, mid, low = split3(tiled)
    group = lax.broadcasted_iota(jnp.int32, tiled.shape, 1) // 16
    zero = jnp.zeros_like(tiled)
    is_high = (group == 0) | (group == 1) | (group == 3)
    is_mid = (group == 2) | (group == 4)
    out = jnp.where(
        is_high,
        high.astype(F32),
        jnp.where(is_mid, mid.astype(F32), jnp.where(group == 5, low.astype(F32), zero)),
    )
    return out.astype(BF16)


def six_right(x):
    high, mid, low = split3(x)
    zero = jnp.zeros_like(high)
    return jnp.concatenate([high, mid, high, low, mid, high, zero, zero], axis=0)


def tile_matrix():
    row = lax.broadcasted_iota(jnp.int32, (16, 128), 0)
    lane = lax.broadcasted_iota(jnp.int32, (16, 128), 1)
    return jnp.where(lane % 16 == row, 1.0, 0.0).astype(F32)


def widened(x, lanes):
    return jnp.concatenate([x, jnp.zeros((x.shape[0], lanes - x.shape[1]), x.dtype)], axis=1)


def lane_window(x, start, width):
    total = x.shape[1]
    if start:
        x = pltpu.roll(x, total - start, 1)
    return x[:, :width]


def at_lanes(x, start):
    return pltpu.roll(x, start, 1) if start else x


def blocks_kernel(coarse_hbm, blocks, coarse, wide, arrived):
    load = pltpu.make_async_copy(coarse_hbm, coarse, arrived.at[0])
    load.start()
    wide[...] = jnp.zeros_like(wide)
    load.wait()
    wide[0:3, :] = coarse[...]
    near = lax.broadcasted_iota(jnp.int32, (8, 128), 1) < 16
    row = lax.broadcasted_iota(jnp.int32, (8, 128), 0)
    unknowns = wide.shape[1]
    grid_rows = blocks.shape[0] // 8
    row_unknowns = unknowns // grid_rows
    for i in range(grid_rows):
        first = row_unknowns * (i - 1)
        span = min(unknowns, 384)
        start = min(max(first // 128, 0) * 128, unknowns - span)
        piece = wide[:, start : start + span]
        if first != start:
            piece = pltpu.roll(piece, (start - first) % span, 1)
        if span < 256:
            piece = widened(piece, 256)
        others = jnp.where(near, piece[:, 128:256], 0.0)
        others = others[0:1] + pltpu.roll(others, 16, 1)[1:2] + pltpu.roll(others, 32, 1)[2:3]
        blocks[8 * i : 8 * i + 8, :] = jnp.where(row == 6, others, pltpu.roll(piece[:, 0:128], 3, 0))


def prepare_kernel(
    count_hbm, slots_hbm, mult_hbm, modes_hbm, schur_hbm,
    place, pick_schur, mode_rows, link_rows,
    buffer, slots, mult, modes, schur, count, arrived,
):
    copies = [
        pltpu.make_async_copy(source, target, arrived.at[n])
        for n, (source, target) in enumerate(
            (
                (count_hbm, count), (slots_hbm, slots), (mult_hbm, mult), (modes_hbm, modes),
                (schur_hbm, schur),
            )
        )
    ]
    for copy in copies:
        copy.start()
    width = slots.shape[1]
    total = 4 * width
    buffer[...] = jnp.zeros_like(buffer)
    lane = lax.broadcasted_iota(jnp.int32, (1, total), 1)
    copies[0].wait()
    copies[1].wait()
    buffer[0:4, 0:width] = slots[...].astype(F32)
    raw = buffer[...]
    slot_row = jnp.zeros((1, total), F32)
    sign_row = jnp.zeros((1, total), F32)
    for f in range(4):
        inside = (lane >= width * f) & (lane < width * f + count[0, f])
        slot_row = jnp.where(inside, at_lanes(raw, width * f)[f : f + 1], slot_row)
        sign_row = jnp.where(inside, SIGNS[f], sign_row)
    copies[2].wait()
    weights = 1.0 / mult[...].astype(F32)
    place_value = placing(slot_row, sign_row)
    place[...] = place_value
    copies[3].wait()
    buffer[...] = jnp.zeros_like(buffer)
    for k in range(modes.shape[0]):
        buffer[k : k + 1, :] = modes[k]
    buffer[3:4, :] = weights
    rows = select_lanes(buffer[...], place_value)
    mode_rows[...] = rows
    buffer[...] = jnp.zeros_like(buffer)
    buffer[0:1, :] = slot_row
    buffer[1:2, :] = sign_row
    buffer[2:3, :] = weights
    buffer[3:4, :] = jnp.abs(rows[3:4])
    link_rows[...] = buffer[...]
    pick_value = picking(jnp.transpose(buffer[...]))
    copies[4].wait()
    pick_schur[...] = dot(pick_value, schur[...]).astype(BF16)


def placing(slot_row, sign_row):
    total = slot_row.shape[1]
    down = lax.broadcasted_iota(jnp.int32, (total, total), 0).astype(F32)
    return jnp.where(down == slot_row, sign_row, 0.0).astype(BF16)


def picking(cols):
    total = cols.shape[0]
    across = lax.broadcasted_iota(jnp.int32, (total, total), 1).astype(F32)
    return jnp.where(across == cols[:, 0:1], cols[:, 1:2], 0.0).astype(BF16)


def precond_kernel(
    gap_down, gap_right, above, left, place, pick_schur, link_rows, mode_rows, saved,
    up_msg, down_msg, left_msg, right_msg, own, residual,
):
    width = above.shape[0]
    columns = jnp.transpose(link_rows[...])
    links = jnp.concatenate([above[...], gap_down[...], left[...], gap_right[...]], axis=0)
    spread = select_rows(place[...], links)
    weighted = (columns[:, 2:3] * spread).astype(BF16)
    picked = columns[:, 3:4] * dot(pick_schur[...], weighted)
    own[...] = picked
    for f, msg in enumerate((up_msg, down_msg, left_msg, right_msg)):
        msg[0:width, :] = picked[width * f : width * f + width]
        rows = lane_window(mode_rows[...], width * f, 256)
        msg[width : width + 8, :] = rows[:, 0:128]
        msg[width + 8 : width + 16, :] = rows[:, 128:256]
    for start, msg in ((0, down_msg), (width, right_msg)):
        rows = lane_window(saved[...], start, 256)
        msg[width + 16 : width + 32, :] = rows[:, 0:128]
        msg[width + 32 : width + 48, :] = rows[:, 128:256]
    residual[0:width, :] = jnp.where(columns[width : 2 * width, 1:2] != 0.0, gap_down[...], 0.0)
    residual[width:, :] = jnp.where(columns[3 * width :, 1:2] != 0.0, gap_right[...], 0.0)


def flex_kernel(
    link_rows, place, flex_hbm, pick_flex_hbm, link_flex_hbm,
    flex, pick_flex, link_flex, arrived,
):
    load = pltpu.make_async_copy(flex_hbm, flex, arrived.at[0])
    load.start()
    pick_value = picking(jnp.transpose(link_rows[...]))
    load.wait()
    rows = dot(pick_value, flex[...]).astype(BF16)
    pick_flex[...] = rows
    store = pltpu.make_async_copy(pick_flex, pick_flex_hbm, arrived.at[1])
    store.start()
    link_flex[...] = dot(rows, place[...]).astype(BF16)
    store_link = pltpu.make_async_copy(link_flex, link_flex_hbm, arrived.at[2])
    store_link.start()
    store.wait()
    store_link.wait()


def coarse_in_kernel(own, above, below, left, right, mode_rows, blocks, precond, coarse):
    width = own.shape[0] // 4
    full = own[...] + jnp.concatenate(
        [above[0:width], below[0:width], left[0:width], right[0:width]], axis=0
    )
    precond[...] = full
    rows = dot_exact(mode_rows[...], full)
    rows = jnp.where(lax.broadcasted_iota(jnp.int32, rows.shape, 0) < 3, rows, 0.0)
    for i in range(coarse.shape[0] // 8):
        coarse[8 * i : 8 * i + 8, :] = rows + blocks[8 * i : 8 * i + 8]


def tables_kernel(
    above, below, left, right, mode_rows, link_rows, saved, images, residual, precond, link_flex_hbm,
    mode_six, search_rows, base, mode_forms,
    link_flex, arrived,
):
    load = pltpu.make_async_copy(link_flex_hbm, link_flex, arrived.at[0])
    load.start()
    total = mode_rows.shape[1]
    width = total // 4
    near = lax.broadcasted_iota(jnp.int32, (1, 256), 1) < width
    used = link_rows[1:2, :] != 0.0
    row = lax.broadcasted_iota(jnp.int32, (16, total), 0)
    mine = jnp.concatenate([mode_rows[...], jnp.zeros((8, total), F32)], axis=0)
    modes = jnp.where(row < 3, mine, 0.0)
    for f, msg in enumerate((above, below, left, right)):
        theirs = jnp.concatenate([msg[width : width + 8], msg[width + 8 : width + 16]], axis=1)
        theirs = at_lanes(widened(jnp.where(near, theirs, 0.0), total), width * f)
        theirs = jnp.concatenate([theirs, jnp.zeros((8, total), F32)], axis=0)
        theirs = jnp.where(row < 3, theirs, 0.0)
        modes = modes + pltpu.roll(theirs, 3 * (1 + f), 0)
    modes = jnp.where(used, modes, 0.0)
    modes_tiled = tiled_columns(modes)
    mode_six[...] = six_left(modes_tiled)
    search = jnp.zeros((16, total), F32)
    for f in range(4):
        if f % 2 == 0:
            msg = above if f == 0 else left
            piece = jnp.concatenate(
                [msg[width + 16 : width + 32], msg[width + 32 : width + 48]], axis=1
            )
        else:
            piece = lane_window(saved[...], 0 if f == 1 else width, 256)
        search = search + at_lanes(widened(jnp.where(near, piece, 0.0), total), width * f)
    search = jnp.where(used, search, 0.0)
    search_rows[...] = search
    lanes = lax.broadcasted_iota(jnp.int32, (16, total), 1)
    image = widened(images[...], total)
    image = jnp.where(
        (lanes >= width) & (lanes < 2 * width),
        at_lanes(image, width),
        jnp.where(lanes >= 3 * width, at_lanes(image, 2 * width), 0.0),
    )
    load.wait()
    flexed = select_lanes(jnp.concatenate([search, modes], axis=0), link_flex[...])
    forms = jnp.concatenate([image, flexed], axis=0)
    full = precond[...]
    base[0:48, :] = dot_exact(forms, full)
    mode_forms[...] = six_left(dot_exact(forms, modes_tiled))
    high, mid, _ = split3(full)
    applied = dot(link_flex[...], jnp.concatenate([high, mid], axis=1))
    square = jnp.sum(full * (applied[:, :128] + applied[:, 128:]), axis=0, keepdims=True)
    products = dot_exact(dot_exact_nt(flexed[0:16], search), tile_matrix())
    group = lax.broadcasted_iota(jnp.int32, (16, 128), 1) // 16
    part = lax.broadcasted_iota(jnp.int32, (16, 128), 0)
    products = jnp.where(group == part % 8, products, 0.0)
    energy = jnp.sum(residual[0:width] * full[width : 2 * width], axis=0, keepdims=True) + jnp.sum(
        residual[width:] * full[3 * width :], axis=0, keepdims=True
    )
    base[48:56, :] = jnp.concatenate(
        [
            energy,
            square,
            jnp.sum(products[0:8], axis=0, keepdims=True),
            jnp.sum(products[8:16], axis=0, keepdims=True),
            jnp.zeros((4, 128), F32),
        ],
        axis=0,
    )


def coarse_kernel(gathered, parts):
    arrived = gathered[...]
    height = arrived.shape[0]
    row = lax.broadcasted_iota(jnp.int32, arrived.shape, 0) % 8
    lane = lax.broadcasted_iota(jnp.int32, arrived.shape, 1)
    coarse_in = jnp.where(row < 3, arrived, 0.0)
    main = jnp.where(row < 3, pltpu.roll(arrived, height - 3, 0), 0.0)
    others = jnp.zeros_like(arrived)
    for k in range(3):
        moved = pltpu.roll(arrived, height - (6 - k), 0)
        if k:
            moved = pltpu.roll(moved, 128 - 16 * k, 1)
        others = others + jnp.where((row == k) & (lane < 16), moved, 0.0)
    product = lax.dot_general(
        jnp.concatenate([main, others], axis=1), coarse_in, (((0,), (0,)), ((), ())),
        precision=HIGHEST, preferred_element_type=F32,
    )
    total = parts.shape[0]
    count = total // 16
    row = lax.broadcasted_iota(jnp.int32, (total, 1), 0)
    j = row >> 4
    part = ((row & 15) * 11) >> 5
    mode = (row & 15) - 3 * part
    down = jnp.where(part == 1, -1, jnp.where(part == 2, 1, 0))
    j = j + jnp.where(part == 3, -1, jnp.where(part == 4, 1, 0))
    valid = (part < 5) & (j >= 0) & (j < count)
    wanted = jnp.where(valid, ((down + 1) * count + j) * 3 + mode, -1)
    at = lax.broadcasted_iota(jnp.int32, (total, 256), 1)
    parts[...] = select_rows(jnp.where(at == wanted, 1.0, 0.0).astype(BF16), product)


def block_sum(ref, height):
    out = ref[0:height]
    for j in range(1, ref.shape[0] // height):
        out = out + ref[height * j : height * j + height]
    return out


def project_kernel(chunk, arrived, base, mode_forms, amplitudes, partial):
    y = block_sum(arrived, 16)
    amplitudes[...] = y
    moved = dot(mode_forms[...], six_right(y))
    linear = base[0:32] - moved[0:32]
    square = jnp.sum(y * (moved[32:48] - 2.0 * base[32:48]), axis=0, keepdims=True)
    row = lax.broadcasted_iota(jnp.int32, (8, 128), 0)
    last = base[48:56] + jnp.where(row == 1, square, 0.0)
    padding = jnp.zeros((partial.shape[0] // 2 - 40, 128), F32)
    full = jnp.concatenate([linear, last, padding], axis=0)
    for j in range(partial.shape[0] // chunk):
        at = chunk * (j // 2)
        partial[chunk * j : chunk * j + chunk, :] = full[at : at + chunk]


def own_rows(x, width):
    return jnp.concatenate([x[width : 2 * width], x[3 * width :]], axis=0)


def lift_kernel(
    amplitudes, precond, mode_six, search_rows, link_rows,
    slot_values, slot_six, link_values, link_six,
):
    links = precond[...] - dot(mode_six[...], six_right(amplitudes[...]))
    width = links.shape[0] // 4
    link_values[...] = own_rows(links, width)
    search = search_rows[...]
    link_six[...] = six_left(own_rows(tiled_columns(search), width))
    place = placing(link_rows[0:1], link_rows[1:2])
    slot_values[...] = select_rows(place, links)
    parts = dot_nt(jnp.concatenate(split3(search), axis=0), place)
    slot_six[...] = six_left(tiled_columns(parts[0:16] + (parts[16:32] + parts[32:48])))


def spread_sum_kernel(height, arrived, partial):
    out = block_sum(arrived, height)
    for i in range(partial.shape[0] // height):
        partial[height * i : height * i + height, :] = out


def search_kernel(sums, slot_values, slot_six, pick_flex, up_msg, left_msg, own):
    width = up_msg.shape[0]
    lifted = slot_values[...] - dot(slot_six[...], six_right(sums[0:16]))
    image = dot(pick_flex[...], lifted.astype(BF16))
    up_msg[...] = image[0:width]
    left_msg[...] = image[2 * width : 3 * width]
    own[...] = own_rows(image, width)


def multiply_kernel(sums, link_values, link_six, multipliers, step):
    intersect = sums[0:16]
    cross = sums[16:32]
    energy = sums[32:33]
    square = sums[33:34]
    group = lax.broadcasted_iota(jnp.int32, (16, 128), 1) // 16
    part = lax.broadcasted_iota(jnp.int32, (16, 128), 0)
    packed = jnp.where(part < 8, sums[34:35], sums[35:36])
    packed = jnp.where(group == part % 8, packed, 0.0)
    products = dot_exact(packed, jnp.concatenate([intersect] * 8, axis=0))
    curvature = square + jnp.sum(intersect * (products - 2.0 * cross), axis=0, keepdims=True)
    size = energy / curvature
    step[...] = jnp.broadcast_to(size, step.shape)
    multipliers[...] = size * (link_values[...] - dot(link_six[...], six_right(intersect)))


def residual_kernel(before, own, below, right, step, residual):
    width = below.shape[0]
    size = step[0:1]
    residual[0:width, :] = before[0:width] - size * (own[0:width] + below[...])
    residual[width:, :] = before[width:] - size * (own[width:] + right[...])


VMEM_LIMIT = 24 * 1024 * 1024
VMEM = pl.BlockSpec(memory_space=pltpu.VMEM)
SMEM = pl.BlockSpec(memory_space=pltpu.SMEM)
HBM = pl.BlockSpec(memory_space=pltpu.HBM)


def call(kernel, inputs, outputs, scalars=0, remote=0, scratch=(), copies=0, hbm_out=(), flops=0):
    out_specs = tuple(HBM if n in hbm_out else VMEM for n in range(len(outputs)))
    outputs = tuple(
        pltpu.HBM(shape, dtype)
        if n in hbm_out
        else jax.ShapeDtypeStruct(shape, dtype)
        for n, (shape, dtype) in enumerate(outputs)
    )
    local = len(inputs) - remote
    inputs = tuple(
        x if n < local else pltpu.with_memory_space_constraint(x, pltpu.HBM)
        for n, x in enumerate(inputs)
    )
    scratch = [
        entry if not isinstance(entry, tuple) else pltpu.VMEM(*entry) for entry in scratch
    ]
    if copies:
        scratch.append(pltpu.SemaphoreType.DMA((copies,)))
    return pl.pallas_call(
        kernel,
        out_shape=outputs,
        in_specs=[SMEM] * scalars + [VMEM] * (len(inputs) - scalars - remote) + [HBM] * remote,
        out_specs=out_specs,
        scratch_shapes=scratch,
        cost_estimate=pl.CostEstimate(flops=flops, transcendentals=0, bytes_accessed=0),
        compiler_params=pltpu.CompilerParams(vmem_limit_bytes=VMEM_LIMIT),
    )(*inputs)


def step(
    gap_load, flexibility, schur_blocks, body_modes, coarse_inverse,
    saved_search, saved_images, face_slots, face_count, multiplicity,
):
    rows = lax.axis_size(GX)
    columns = lax.axis_size(GY)
    gap = gap_load[0, 0]
    flex = flexibility[0, 0]
    modes = jnp.transpose(body_modes, (0, 2, 1, 3))[0]
    saved = saved_search[0, 0]
    images = saved_images[0, 0]
    slots = face_slots[0, 0]
    count = face_count[0]
    width = slots.shape[1]
    total = 4 * width
    cases = gap.shape[1]
    unknowns = coarse_inverse.shape[1]
    big = (total, total)
    cube = 2 * total**3
    gap_down = gap[:width]
    gap_right = gap[width:]
    above = shifted(gap_down, GX, 1)
    left = shifted(gap_right, GY, 1)
    (blocks,) = call(
        blocks_kernel,
        (coarse_inverse,),
        (((8 * rows, 128), F32),),
        remote=1,
        scratch=((coarse_inverse.shape, F32), ((8, unknowns), F32)),
        copies=1,
        flops=cube // 64,
    )
    place, pick_schur, mode_rows, link_rows = call(
        prepare_kernel,
        (count, slots, multiplicity[0], modes, schur_blocks[0, 0]),
        (
            (big, BF16), (big, BF16), ((8, total), F32), ((8, total), F32),
        ),
        remote=5,
        scratch=(
            ((8, total), F32), (slots.shape, jnp.int32), ((1, total), jnp.int32), (modes.shape, F32),
            (big, BF16), pltpu.SMEM((1, 4), jnp.int32),
        ),
        copies=5,
        flops=cube,
    )
    up_msg, down_msg, left_msg, right_msg, own, residual = call(
        precond_kernel,
        (gap_down, gap_right, above, left, place, pick_schur, link_rows, mode_rows, saved),
        tuple(((width + extra, cases), F32) for extra in (16, 48, 16, 48))
        + (((total, cases), F32), ((2 * width, cases), F32)),
        flops=cube // 2,
    )
    from_above = shifted(down_msg, GX, 1)
    from_below = shifted(up_msg, GX, -1)
    from_left = shifted(right_msg, GY, 1)
    from_right = shifted(left_msg, GY, -1)
    precond, coarse_in = call(
        coarse_in_kernel,
        (own, from_above, from_below, from_left, from_right, mode_rows, blocks),
        (((total, cases), F32), ((8 * rows, cases), F32)),
        flops=cube // 16,
    )
    gathered = lax.all_to_all(coarse_in, GX, 0, 0, tiled=True)
    pick_flex, link_flex = call(
        flex_kernel,
        (link_rows, place, flex),
        ((big, BF16), (big, BF16)),
        remote=1,
        scratch=((big, BF16), (big, BF16), (big, BF16)),
        copies=3,
        hbm_out=(0, 1),
        flops=2 * cube,
    )
    (parts,) = call(coarse_kernel, (gathered,), (((16 * columns, cases), F32),), flops=cube // 8)
    parts = lax.all_to_all(parts, GY, 0, 0, tiled=True)
    mode_six, search_rows, base, mode_forms = call(
        tables_kernel,
        (
            from_above, from_below, from_left, from_right, mode_rows, link_rows, saved, images,
            residual, precond, link_flex,
        ),
        (((total, 128), BF16), ((16, total), F32), ((56, cases), F32), ((48, 128), BF16)),
        remote=1,
        scratch=((big, BF16),),
        copies=1,
        flops=cube,
    )
    pairs = columns // 2
    chunk = -(-(-(-40 // pairs)) // 8) * 8
    amplitudes, partial = call(
        functools.partial(project_kernel, chunk),
        (parts, base, mode_forms),
        (((16, cases), F32), ((chunk * columns, cases), F32)),
        flops=cube // 64,
    )
    slot_values, slot_six, link_values, link_six = call(
        lift_kernel,
        (amplitudes, precond, mode_six, search_rows, link_rows),
        (
            ((total, cases), F32), ((total, 128), BF16), ((2 * width, cases), F32),
            ((2 * width, 128), BF16),
        ),
        flops=cube,
    )
    for axis, following in ((GY, rows), (GX, pairs)):
        partial = lax.all_to_all(partial, axis, 0, 0, tiled=True)
        (partial,) = call(
            functools.partial(spread_sum_kernel, chunk),
            (partial,),
            (((chunk * following, cases), F32),),
            flops=cube // 64,
        )
    sums = lax.all_to_all(partial, GY[0], 0, 0, tiled=True)
    up_msg, left_msg, own = call(
        search_kernel,
        (sums, slot_values, slot_six, pick_flex),
        (((width, cases), F32), ((width, cases), F32), ((2 * width, cases), F32)),
        flops=cube // 2,
    )
    from_below = shifted(up_msg, GX, -1)
    from_right = shifted(left_msg, GY, -1)
    multipliers, step = call(
        multiply_kernel,
        (sums, link_values, link_six),
        (((2 * width, cases), F32), ((8, cases), F32)),
        flops=cube // 64,
    )
    (residual,) = call(
        residual_kernel,
        (residual, own, from_below, from_right, step),
        (((2 * width, cases), F32),),
        flops=cube // 64,
    )
    return (multipliers[None, None], residual[None, None])


def split_shape(mesh):
    rows, columns = (mesh.devices.shape[0], mesh.devices.shape[1])
    inner = 4 if rows % 4 == 0 and rows > 4 else 2
    return (rows // inner, inner, columns // 2, 2)


def solution(mesh):
    split = Mesh(mesh.devices.reshape(split_shape(mesh)), GX_GY)
    placed = (
        P(GX, GY, None, None),
        P(GX, GY, None, None),
        P(GX, GY, None, None),
        P(GX, GY, None, None),
        P(GX_GY, None),
        P(GX, GY, None, None),
        P(GX, GY, None, None),
        P(GX, GY, None, None),
        P(GX, GY, None),
        P(GX, GY, None),
    )
    return jax.shard_map(
        step,
        mesh=split,
        in_specs=placed,
        out_specs=(P(GX, GY, None, None), P(GX, GY, None, None)),
        check_vma=False,
    )
```

```python
import functools

import jax
import jax.numpy as jnp
from jax import lax
from jax.experimental import pallas as pl
from jax.experimental.pallas import tpu as pltpu
from jax.sharding import Mesh
from jax.sharding import PartitionSpec as P


GX = ("gx_0", "gx_1")
GY = ("gy_0", "gy_1")
GX_GY = ("gx_0", "gx_1", "gy_0", "gy_1")

F32 = jnp.float32
BF16 = jnp.bfloat16
HIGHEST = lax.Precision.HIGHEST
SIGNS = (-1.0, 1.0, -1.0, 1.0)


def shifted(value, axis, steps):
    count = lax.axis_size(axis)
    initial, last = (max(0, -steps), min(count, count - steps))
    return lax.ppermute(value, axis, [(source, source + steps) for source in range(initial, last)])


def swapped(value, axis, first):
    count = lax.axis_size(axis)
    pairs = [(low, low + 1) for low in range(first, count - 1, 2)]
    return lax.ppermute(value, axis, pairs + [(high, low) for low, high in pairs])


def split3(x):
    high = x.astype(BF16)
    rest = x - high.astype(F32)
    mid = rest.astype(BF16)
    low = (rest - mid.astype(F32)).astype(BF16)
    return high, mid, low


def dot(a, b):
    return lax.dot_general(a, b, (((1,), (0,)), ((), ())), preferred_element_type=F32)


def dot_nt(a, b):
    return lax.dot_general(a, b, (((1,), (1,)), ((), ())), preferred_element_type=F32)


def dot_exact(a, b):
    return lax.dot_general(
        a, b, (((1,), (0,)), ((), ())), precision=HIGHEST, preferred_element_type=F32
    )


def dot_exact_nt(a, b):
    return lax.dot_general(
        a, b, (((1,), (1,)), ((), ())), precision=HIGHEST, preferred_element_type=F32
    )


def tiled_columns(rows):
    return lax.dot_general(
        rows, tile_matrix(), (((0,), (0,)), ((), ())), precision=HIGHEST, preferred_element_type=F32
    )


def select_rows(selection, x):
    width = x.shape[1]
    out = dot(selection, jnp.concatenate(split3(x), axis=1))
    return out[:, :width] + (out[:, width : 2 * width] + out[:, 2 * width :])


def select_lanes(x, selection):
    rows = x.shape[0]
    out = dot(jnp.concatenate(split3(x), axis=0), selection)
    return out[:rows] + (out[rows : 2 * rows] + out[2 * rows :])


def six_left(tiled):
    high, mid, low = split3(tiled)
    group = lax.broadcasted_iota(jnp.int32, tiled.shape, 1) // 16
    zero = jnp.zeros_like(tiled)
    is_high = (group == 0) | (group == 1) | (group == 3)
    is_mid = (group == 2) | (group == 4)
    out = jnp.where(
        is_high,
        high.astype(F32),
        jnp.where(is_mid, mid.astype(F32), jnp.where(group == 5, low.astype(F32), zero)),
    )
    return out.astype(BF16)


def six_right(x):
    high, mid, low = split3(x)
    zero = jnp.zeros_like(high)
    return jnp.concatenate([high, mid, high, low, mid, high, zero, zero], axis=0)


def tile_matrix():
    row = lax.broadcasted_iota(jnp.int32, (16, 128), 0)
    lane = lax.broadcasted_iota(jnp.int32, (16, 128), 1)
    return jnp.where(lane % 16 == row, 1.0, 0.0).astype(F32)


def widened(x, lanes):
    return jnp.concatenate([x, jnp.zeros((x.shape[0], lanes - x.shape[1]), x.dtype)], axis=1)


def lane_window(x, start, width):
    total = x.shape[1]
    if start:
        x = pltpu.roll(x, total - start, 1)
    return x[:, :width]


def at_lanes(x, start):
    return pltpu.roll(x, start, 1) if start else x


def blocks_kernel(coarse_hbm, blocks, coarse, wide, arrived):
    load = pltpu.make_async_copy(coarse_hbm, coarse, arrived.at[0])
    load.start()
    wide[...] = jnp.zeros_like(wide)
    load.wait()
    wide[0:3, :] = coarse[...]
    near = lax.broadcasted_iota(jnp.int32, (8, 128), 1) < 16
    row = lax.broadcasted_iota(jnp.int32, (8, 128), 0)
    unknowns = wide.shape[1]
    grid_rows = blocks.shape[0] // 8
    row_unknowns = unknowns // grid_rows
    for i in range(grid_rows):
        first = row_unknowns * (i - 1)
        span = min(unknowns, 384)
        start = min(max(first // 128, 0) * 128, unknowns - span)
        piece = wide[:, start : start + span]
        if first != start:
            piece = pltpu.roll(piece, (start - first) % span, 1)
        if span < 256:
            piece = widened(piece, 256)
        others = jnp.where(near, piece[:, 128:256], 0.0)
        others = others[0:1] + pltpu.roll(others, 16, 1)[1:2] + pltpu.roll(others, 32, 1)[2:3]
        blocks[8 * i : 8 * i + 8, :] = jnp.where(row == 6, others, pltpu.roll(piece[:, 0:128], 3, 0))


def prepare_kernel(
    count_hbm, slots_hbm, mult_hbm, modes_hbm, schur_hbm,
    place, pick_schur, mode_rows, link_rows,
    buffer, slots, mult, modes, schur, count, arrived,
):
    copies = [
        pltpu.make_async_copy(source, target, arrived.at[n])
        for n, (source, target) in enumerate(
            (
                (count_hbm, count), (slots_hbm, slots), (mult_hbm, mult), (modes_hbm, modes),
                (schur_hbm, schur),
            )
        )
    ]
    for copy in copies:
        copy.start()
    width = slots.shape[1]
    total = 4 * width
    buffer[...] = jnp.zeros_like(buffer)
    lane = lax.broadcasted_iota(jnp.int32, (1, total), 1)
    copies[0].wait()
    copies[1].wait()
    buffer[0:4, 0:width] = slots[...].astype(F32)
    raw = buffer[...]
    slot_row = jnp.zeros((1, total), F32)
    sign_row = jnp.zeros((1, total), F32)
    for f in range(4):
        inside = (lane >= width * f) & (lane < width * f + count[0, f])
        slot_row = jnp.where(inside, at_lanes(raw, width * f)[f : f + 1], slot_row)
        sign_row = jnp.where(inside, SIGNS[f], sign_row)
    copies[2].wait()
    weights = 1.0 / mult[...].astype(F32)
    place_value = placing(slot_row, sign_row)
    place[...] = place_value
    copies[3].wait()
    buffer[...] = jnp.zeros_like(buffer)
    for k in range(modes.shape[0]):
        buffer[k : k + 1, :] = modes[k]
    buffer[3:4, :] = weights
    rows = select_lanes(buffer[...], place_value)
    mode_rows[...] = rows
    buffer[...] = jnp.zeros_like(buffer)
    buffer[0:1, :] = slot_row
    buffer[1:2, :] = sign_row
    buffer[2:3, :] = weights
    buffer[3:4, :] = jnp.abs(rows[3:4])
    link_rows[...] = buffer[...]
    pick_value = picking(jnp.transpose(buffer[...]))
    copies[4].wait()
    pick_schur[...] = dot(pick_value, schur[...]).astype(BF16)


def placing(slot_row, sign_row):
    total = slot_row.shape[1]
    down = lax.broadcasted_iota(jnp.int32, (total, total), 0).astype(F32)
    return jnp.where(down == slot_row, sign_row, 0.0).astype(BF16)


def picking(cols):
    total = cols.shape[0]
    across = lax.broadcasted_iota(jnp.int32, (total, total), 1).astype(F32)
    return jnp.where(across == cols[:, 0:1], cols[:, 1:2], 0.0).astype(BF16)


def precond_kernel(
    odd_x, odd_y, gap_down, gap_right, above, left, place, pick_schur, link_rows, mode_rows, saved,
    first_x, second_x, first_y, second_y, own, residual,
):
    width = above.shape[0]
    total = 4 * width
    columns = jnp.transpose(link_rows[...])
    links = jnp.concatenate([above[...], gap_down[...], left[...], gap_right[...]], axis=0)
    spread = select_rows(place[...], links)
    weighted = (columns[:, 2:3] * spread).astype(BF16)
    own[...] = columns[:, 3:4] * dot(pick_schur[...], weighted)
    for face, start, msg in (
        (1 - odd_x[0], 0, first_x),
        (odd_x[0], 0, second_x),
        (3 - odd_y[0], width, first_y),
        (2 + odd_y[0], width, second_y),
    ):
        msg[0:width, :] = own[pl.ds(pl.multiple_of(width * face, 8), width), :]
        rows = pltpu.roll(mode_rows[...], jnp.where(face == 0, 0, total - width * face), 1)
        msg[width : width + 8, :] = rows[:, 0:128]
        msg[width + 8 : width + 16, :] = rows[:, 128:256]
        rows = lane_window(saved[...], start, 256)
        msg[width + 16 : width + 32, :] = rows[:, 0:128]
        msg[width + 32 : width + 48, :] = rows[:, 128:256]
    residual[0:width, :] = jnp.where(columns[width : 2 * width, 1:2] != 0.0, gap_down[...], 0.0)
    residual[width:, :] = jnp.where(columns[3 * width :, 1:2] != 0.0, gap_right[...], 0.0)


def four_neighbours(odd_x, odd_y, first_x, second_x, first_y, second_y):
    even_x = odd_x[0] == 0
    even_y = odd_y[0] == 0
    return (
        jnp.where(even_x, second_x, first_x),
        jnp.where(even_x, first_x, second_x),
        jnp.where(even_y, second_y, first_y),
        jnp.where(even_y, first_y, second_y),
    )


def flex_kernel(
    link_rows, place, flex_hbm, pick_flex_hbm, link_flex_hbm,
    flex, pick_flex, link_flex, arrived,
):
    load = pltpu.make_async_copy(flex_hbm, flex, arrived.at[0])
    load.start()
    pick_value = picking(jnp.transpose(link_rows[...]))
    load.wait()
    rows = dot(pick_value, flex[...]).astype(BF16)
    pick_flex[...] = rows
    store = pltpu.make_async_copy(pick_flex, pick_flex_hbm, arrived.at[1])
    store.start()
    link_flex[...] = dot(rows, place[...]).astype(BF16)
    store_link = pltpu.make_async_copy(link_flex, link_flex_hbm, arrived.at[2])
    store_link.start()
    store.wait()
    store_link.wait()


def coarse_in_kernel(
    odd_x, odd_y, own, first_x, second_x, first_y, second_y, mode_rows, blocks, precond, coarse
):
    width = own.shape[0] // 4
    full = own[...] + jnp.concatenate(
        four_neighbours(
            odd_x, odd_y, first_x[0:width], second_x[0:width], first_y[0:width], second_y[0:width]
        ),
        axis=0,
    )
    precond[...] = full
    rows = dot_exact(mode_rows[...], full)
    rows = jnp.where(lax.broadcasted_iota(jnp.int32, rows.shape, 0) < 3, rows, 0.0)
    for i in range(coarse.shape[0] // 8):
        coarse[8 * i : 8 * i + 8, :] = rows + blocks[8 * i : 8 * i + 8]


def tables_kernel(
    odd_x, odd_y, first_x, second_x, first_y, second_y,
    mode_rows, link_rows, saved, images, residual, precond, link_flex_hbm,
    mode_six, search_rows, base, mode_forms,
    link_flex, arrived,
):
    load = pltpu.make_async_copy(link_flex_hbm, link_flex, arrived.at[0])
    load.start()
    total = mode_rows.shape[1]
    width = total // 4
    near = lax.broadcasted_iota(jnp.int32, (1, 256), 1) < width
    messages = four_neighbours(
        odd_x, odd_y, first_x[width:], second_x[width:], first_y[width:], second_y[width:]
    )
    used = link_rows[1:2, :] != 0.0
    row = lax.broadcasted_iota(jnp.int32, (16, total), 0)
    mine = jnp.concatenate([mode_rows[...], jnp.zeros((8, total), F32)], axis=0)
    modes = jnp.where(row < 3, mine, 0.0)
    for f, msg in enumerate(messages):
        theirs = jnp.concatenate([msg[0:8], msg[8:16]], axis=1)
        theirs = at_lanes(widened(jnp.where(near, theirs, 0.0), total), width * f)
        theirs = jnp.concatenate([theirs, jnp.zeros((8, total), F32)], axis=0)
        theirs = jnp.where(row < 3, theirs, 0.0)
        modes = modes + pltpu.roll(theirs, 3 * (1 + f), 0)
    modes = jnp.where(used, modes, 0.0)
    modes_tiled = tiled_columns(modes)
    mode_six[...] = six_left(modes_tiled)
    search = jnp.zeros((16, total), F32)
    for f in range(4):
        if f % 2 == 0:
            piece = jnp.concatenate([messages[f][16:32], messages[f][32:48]], axis=1)
        else:
            piece = lane_window(saved[...], 0 if f == 1 else width, 256)
        search = search + at_lanes(widened(jnp.where(near, piece, 0.0), total), width * f)
    search = jnp.where(used, search, 0.0)
    search_rows[...] = search
    lanes = lax.broadcasted_iota(jnp.int32, (16, total), 1)
    image = widened(images[...], total)
    image = jnp.where(
        (lanes >= width) & (lanes < 2 * width),
        at_lanes(image, width),
        jnp.where(lanes >= 3 * width, at_lanes(image, 2 * width), 0.0),
    )
    load.wait()
    flexed = select_lanes(jnp.concatenate([search, modes], axis=0), link_flex[...])
    forms = jnp.concatenate([image, flexed], axis=0)
    full = precond[...]
    base[0:48, :] = dot_exact(forms, full)
    mode_forms[...] = six_left(dot_exact(forms, modes_tiled))
    high, mid, _ = split3(full)
    applied = dot(link_flex[...], jnp.concatenate([high, mid], axis=1))
    square = jnp.sum(full * (applied[:, :128] + applied[:, 128:]), axis=0, keepdims=True)
    products = dot_exact(dot_exact_nt(flexed[0:16], search), tile_matrix())
    group = lax.broadcasted_iota(jnp.int32, (16, 128), 1) // 16
    part = lax.broadcasted_iota(jnp.int32, (16, 128), 0)
    products = jnp.where(group == part % 8, products, 0.0)
    energy = jnp.sum(residual[0:width] * full[width : 2 * width], axis=0, keepdims=True) + jnp.sum(
        residual[width:] * full[3 * width :], axis=0, keepdims=True
    )
    base[48:56, :] = jnp.concatenate(
        [
            energy,
            square,
            jnp.sum(products[0:8], axis=0, keepdims=True),
            jnp.sum(products[8:16], axis=0, keepdims=True),
            jnp.zeros((4, 128), F32),
        ],
        axis=0,
    )


def coarse_kernel(gathered, parts):
    arrived = gathered[...]
    height = arrived.shape[0]
    row = lax.broadcasted_iota(jnp.int32, arrived.shape, 0) % 8
    lane = lax.broadcasted_iota(jnp.int32, arrived.shape, 1)
    coarse_in = jnp.where(row < 3, arrived, 0.0)
    main = jnp.where(row < 3, pltpu.roll(arrived, height - 3, 0), 0.0)
    others = jnp.zeros_like(arrived)
    for k in range(3):
        moved = pltpu.roll(arrived, height - (6 - k), 0)
        if k:
            moved = pltpu.roll(moved, 128 - 16 * k, 1)
        others = others + jnp.where((row == k) & (lane < 16), moved, 0.0)
    product = lax.dot_general(
        jnp.concatenate([main, others], axis=1), coarse_in, (((0,), (0,)), ((), ())),
        precision=HIGHEST, preferred_element_type=F32,
    )
    total = parts.shape[0]
    count = total // 16
    row = lax.broadcasted_iota(jnp.int32, (total, 1), 0)
    j = row >> 4
    part = ((row & 15) * 11) >> 5
    mode = (row & 15) - 3 * part
    down = jnp.where(part == 1, -1, jnp.where(part == 2, 1, 0))
    j = j + jnp.where(part == 3, -1, jnp.where(part == 4, 1, 0))
    valid = (part < 5) & (j >= 0) & (j < count)
    wanted = jnp.where(valid, ((down + 1) * count + j) * 3 + mode, -1)
    at = lax.broadcasted_iota(jnp.int32, (total, 256), 1)
    parts[...] = select_rows(jnp.where(at == wanted, 1.0, 0.0).astype(BF16), product)


def block_sum(ref, height):
    out = ref[0:height]
    for j in range(1, ref.shape[0] // height):
        out = out + ref[height * j : height * j + height]
    return out


def project_kernel(chunk, arrived, base, mode_forms, amplitudes, partial):
    y = block_sum(arrived, 16)
    amplitudes[...] = y
    moved = dot(mode_forms[...], six_right(y))
    linear = base[0:32] - moved[0:32]
    square = jnp.sum(y * (moved[32:48] - 2.0 * base[32:48]), axis=0, keepdims=True)
    row = lax.broadcasted_iota(jnp.int32, (8, 128), 0)
    last = base[48:56] + jnp.where(row == 1, square, 0.0)
    padding = jnp.zeros((partial.shape[0] // 2 - 40, 128), F32)
    full = jnp.concatenate([linear, last, padding], axis=0)
    for j in range(partial.shape[0] // chunk):
        at = chunk * (j // 2)
        partial[chunk * j : chunk * j + chunk, :] = full[at : at + chunk]


def own_rows(x, width):
    return jnp.concatenate([x[width : 2 * width], x[3 * width :]], axis=0)


def lift_kernel(
    amplitudes, precond, mode_six, search_rows, link_rows,
    slot_values, slot_six, link_values, link_six,
):
    links = precond[...] - dot(mode_six[...], six_right(amplitudes[...]))
    width = links.shape[0] // 4
    link_values[...] = own_rows(links, width)
    search = search_rows[...]
    link_six[...] = six_left(own_rows(tiled_columns(search), width))
    place = placing(link_rows[0:1], link_rows[1:2])
    slot_values[...] = select_rows(place, links)
    parts = dot_nt(jnp.concatenate(split3(search), axis=0), place)
    slot_six[...] = six_left(tiled_columns(parts[0:16] + (parts[16:32] + parts[32:48])))


def spread_sum_kernel(height, arrived, partial):
    out = block_sum(arrived, height)
    for i in range(partial.shape[0] // height):
        partial[height * i : height * i + height, :] = out


def search_kernel(sums, slot_values, slot_six, pick_flex, up_msg, left_msg, own):
    width = up_msg.shape[0]
    lifted = slot_values[...] - dot(slot_six[...], six_right(sums[0:16]))
    image = dot(pick_flex[...], lifted.astype(BF16))
    up_msg[...] = image[0:width]
    left_msg[...] = image[2 * width : 3 * width]
    own[...] = own_rows(image, width)


def multiply_kernel(sums, link_values, link_six, multipliers, step):
    intersect = sums[0:16]
    cross = sums[16:32]
    energy = sums[32:33]
    square = sums[33:34]
    group = lax.broadcasted_iota(jnp.int32, (16, 128), 1) // 16
    part = lax.broadcasted_iota(jnp.int32, (16, 128), 0)
    packed = jnp.where(part < 8, sums[34:35], sums[35:36])
    packed = jnp.where(group == part % 8, packed, 0.0)
    products = dot_exact(packed, jnp.concatenate([intersect] * 8, axis=0))
    curvature = square + jnp.sum(intersect * (products - 2.0 * cross), axis=0, keepdims=True)
    size = energy / curvature
    step[...] = jnp.broadcast_to(size, step.shape)
    multipliers[...] = size * (link_values[...] - dot(link_six[...], six_right(intersect)))


def residual_kernel(before, own, below, right, step, residual):
    width = below.shape[0]
    size = step[0:1]
    residual[0:width, :] = before[0:width] - size * (own[0:width] + below[...])
    residual[width:, :] = before[width:] - size * (own[width:] + right[...])


VMEM_LIMIT = 24 * 1024 * 1024
VMEM = pl.BlockSpec(memory_space=pltpu.VMEM)
SMEM = pl.BlockSpec(memory_space=pltpu.SMEM)
HBM = pl.BlockSpec(memory_space=pltpu.HBM)


def call(kernel, inputs, outputs, scalars=0, remote=0, scratch=(), copies=0, hbm_out=(), flops=0):
    out_specs = tuple(HBM if n in hbm_out else VMEM for n in range(len(outputs)))
    outputs = tuple(
        pltpu.HBM(shape, dtype)
        if n in hbm_out
        else jax.ShapeDtypeStruct(shape, dtype)
        for n, (shape, dtype) in enumerate(outputs)
    )
    local = len(inputs) - remote
    inputs = tuple(
        x if n < local else pltpu.with_memory_space_constraint(x, pltpu.HBM)
        for n, x in enumerate(inputs)
    )
    scratch = [
        entry if not isinstance(entry, tuple) else pltpu.VMEM(*entry) for entry in scratch
    ]
    if copies:
        scratch.append(pltpu.SemaphoreType.DMA((copies,)))
    return pl.pallas_call(
        kernel,
        out_shape=outputs,
        in_specs=[SMEM] * scalars + [VMEM] * (len(inputs) - scalars - remote) + [HBM] * remote,
        out_specs=out_specs,
        scratch_shapes=scratch,
        cost_estimate=pl.CostEstimate(flops=flops, transcendentals=0, bytes_accessed=0),
        compiler_params=pltpu.CompilerParams(vmem_limit_bytes=VMEM_LIMIT),
    )(*inputs)


def step(
    gap_load, flexibility, schur_blocks, body_modes, coarse_inverse,
    saved_search, saved_images, face_slots, face_count, multiplicity,
):
    rows = lax.axis_size(GX)
    columns = lax.axis_size(GY)
    gap = gap_load[0, 0]
    flex = flexibility[0, 0]
    modes = jnp.transpose(body_modes, (0, 2, 1, 3))[0]
    saved = saved_search[0, 0]
    images = saved_images[0, 0]
    slots = face_slots[0, 0]
    count = face_count[0]
    width = slots.shape[1]
    total = 4 * width
    cases = gap.shape[1]
    unknowns = coarse_inverse.shape[1]
    big = (total, total)
    cube = 2 * total**3
    gap_down = gap[:width]
    gap_right = gap[width:]
    above = shifted(gap_down, GX, 1)
    left = shifted(gap_right, GY, 1)
    place, pick_schur, mode_rows, link_rows = call(
        prepare_kernel,
        (count, slots, multiplicity[0], modes, schur_blocks[0, 0]),
        (
            (big, BF16), (big, BF16), ((8, total), F32), ((8, total), F32),
        ),
        remote=5,
        scratch=(
            ((8, total), F32), (slots.shape, jnp.int32), ((1, total), jnp.int32), (modes.shape, F32),
            (big, BF16), pltpu.SMEM((1, 4), jnp.int32),
        ),
        copies=5,
        flops=cube,
    )
    odd_x = (lax.axis_index(GX) % 2).reshape(1)
    odd_y = (lax.axis_index(GY) % 2).reshape(1)
    first_x, second_x, first_y, second_y, own, residual = call(
        precond_kernel,
        (odd_x, odd_y, gap_down, gap_right, above, left, place, pick_schur, link_rows, mode_rows, saved),
        (((width + 48, cases), F32),) * 4 + (((total, cases), F32), ((2 * width, cases), F32)),
        scalars=2,
        flops=cube // 2,
    )
    first_x = swapped(first_x, GX, 0)
    second_x = swapped(second_x, GX, 1)
    first_y = swapped(first_y, GY, 0)
    second_y = swapped(second_y, GY, 1)
    messages = (first_x, second_x, first_y, second_y)
    (blocks,) = call(
        blocks_kernel,
        (coarse_inverse,),
        (((8 * rows, 128), F32),),
        remote=1,
        scratch=((coarse_inverse.shape, F32), ((8, unknowns), F32)),
        copies=1,
        flops=cube // 64,
    )
    precond, coarse_in = call(
        coarse_in_kernel,
        (odd_x, odd_y, own, *messages, mode_rows, blocks),
        (((total, cases), F32), ((8 * rows, cases), F32)),
        scalars=2,
        flops=cube // 16,
    )
    gathered = lax.all_to_all(coarse_in, GX, 0, 0, tiled=True)
    pick_flex, link_flex = call(
        flex_kernel,
        (link_rows, place, flex),
        ((big, BF16), (big, BF16)),
        remote=1,
        scratch=((big, BF16), (big, BF16), (big, BF16)),
        copies=3,
        hbm_out=(0, 1),
        flops=2 * cube,
    )
    (parts,) = call(coarse_kernel, (gathered,), (((16 * columns, cases), F32),), flops=cube // 8)
    parts = lax.all_to_all(parts, GY, 0, 0, tiled=True)
    mode_six, search_rows, base, mode_forms = call(
        tables_kernel,
        (odd_x, odd_y, *messages, mode_rows, link_rows, saved, images, residual, precond, link_flex),
        (((total, 128), BF16), ((16, total), F32), ((56, cases), F32), ((48, 128), BF16)),
        scalars=2,
        remote=1,
        scratch=((big, BF16),),
        copies=1,
        flops=cube,
    )
    pairs = columns // 2
    chunk = -(-(-(-40 // pairs)) // 8) * 8
    amplitudes, partial = call(
        functools.partial(project_kernel, chunk),
        (parts, base, mode_forms),
        (((16, cases), F32), ((chunk * columns, cases), F32)),
        flops=cube // 64,
    )
    slot_values, slot_six, link_values, link_six = call(
        lift_kernel,
        (amplitudes, precond, mode_six, search_rows, link_rows),
        (
            ((total, cases), F32), ((total, 128), BF16), ((2 * width, cases), F32),
            ((2 * width, 128), BF16),
        ),
        flops=cube,
    )
    for axis, following in ((GY, rows), (GX, pairs)):
        partial = lax.all_to_all(partial, axis, 0, 0, tiled=True)
        (partial,) = call(
            functools.partial(spread_sum_kernel, chunk),
            (partial,),
            (((chunk * following, cases), F32),),
            flops=cube // 64,
        )
    sums = lax.all_to_all(partial, GY[0], 0, 0, tiled=True)
    up_msg, left_msg, own = call(
        search_kernel,
        (sums, slot_values, slot_six, pick_flex),
        (((width, cases), F32), ((width, cases), F32), ((2 * width, cases), F32)),
        flops=cube // 2,
    )
    from_below = shifted(up_msg, GX, -1)
    from_right = shifted(left_msg, GY, -1)
    multipliers, step = call(
        multiply_kernel,
        (sums, link_values, link_six),
        (((2 * width, cases), F32), ((8, cases), F32)),
        flops=cube // 64,
    )
    (residual,) = call(
        residual_kernel,
        (residual, own, from_below, from_right, step),
        (((2 * width, cases), F32),),
        flops=cube // 64,
    )
    return (multipliers[None, None], residual[None, None])


def split_shape(mesh):
    rows, columns = (mesh.devices.shape[0], mesh.devices.shape[1])
    inner = 4 if rows % 4 == 0 and rows > 4 else 2
    return (rows // inner, inner, columns // 2, 2)


def solution(mesh):
    split = Mesh(mesh.devices.reshape(split_shape(mesh)), GX_GY)
    placed = (
        P(GX, GY, None, None),
        P(GX, GY, None, None),
        P(GX, GY, None, None),
        P(GX, GY, None, None),
        P(GX_GY, None),
        P(GX, GY, None, None),
        P(GX, GY, None, None),
        P(GX, GY, None, None),
        P(GX, GY, None),
        P(GX, GY, None),
    )
    return jax.shard_map(
        step,
        mesh=split,
        in_specs=placed,
        out_specs=(P(GX, GY, None, None), P(GX, GY, None, None)),
        check_vma=False,
    )
```

```python
import functools

import jax
import jax.numpy as jnp
from jax import lax
from jax.experimental import pallas as pl
from jax.experimental.pallas import tpu as pltpu
from jax.sharding import Mesh
from jax.sharding import PartitionSpec as P


GX = ("gx_0", "gx_1")
GY = ("gy_0", "gy_1")
GX_GY = ("gx_0", "gx_1", "gy_0", "gy_1")

F32 = jnp.float32
BF16 = jnp.bfloat16
HIGHEST = lax.Precision.HIGHEST
SIGNS = (-1.0, 1.0, -1.0, 1.0)


def shifted(value, axis, steps):
    count = lax.axis_size(axis)
    initial, last = (max(0, -steps), min(count, count - steps))
    return lax.ppermute(value, axis, [(source, source + steps) for source in range(initial, last)])


def swapped(value, axis, first):
    count = lax.axis_size(axis)
    pairs = [(low, low + 1) for low in range(first, count - 1, 2)]
    return lax.ppermute(value, axis, pairs + [(high, low) for low, high in pairs])


def split3(x):
    high = x.astype(BF16)
    rest = x - high.astype(F32)
    mid = rest.astype(BF16)
    low = (rest - mid.astype(F32)).astype(BF16)
    return high, mid, low


def dot(a, b):
    return lax.dot_general(a, b, (((1,), (0,)), ((), ())), preferred_element_type=F32)


def dot_nt(a, b):
    return lax.dot_general(a, b, (((1,), (1,)), ((), ())), preferred_element_type=F32)


def dot_exact(a, b):
    return lax.dot_general(
        a, b, (((1,), (0,)), ((), ())), precision=HIGHEST, preferred_element_type=F32
    )


def dot_exact_nt(a, b):
    return lax.dot_general(
        a, b, (((1,), (1,)), ((), ())), precision=HIGHEST, preferred_element_type=F32
    )


def tiled_columns(rows):
    return lax.dot_general(
        rows, tile_matrix(), (((0,), (0,)), ((), ())), precision=HIGHEST, preferred_element_type=F32
    )


def select_rows(selection, x):
    width = x.shape[1]
    out = dot(selection, jnp.concatenate(split3(x), axis=1))
    return out[:, :width] + (out[:, width : 2 * width] + out[:, 2 * width :])


def select_lanes(x, selection):
    rows = x.shape[0]
    out = dot(jnp.concatenate(split3(x), axis=0), selection)
    return out[:rows] + (out[rows : 2 * rows] + out[2 * rows :])


def six_left(tiled):
    high, mid, low = split3(tiled)
    group = lax.broadcasted_iota(jnp.int32, tiled.shape, 1) // 16
    zero = jnp.zeros_like(tiled)
    is_high = (group == 0) | (group == 1) | (group == 3)
    is_mid = (group == 2) | (group == 4)
    out = jnp.where(
        is_high,
        high.astype(F32),
        jnp.where(is_mid, mid.astype(F32), jnp.where(group == 5, low.astype(F32), zero)),
    )
    return out.astype(BF16)


def six_right(x):
    high, mid, low = split3(x)
    zero = jnp.zeros_like(high)
    return jnp.concatenate([high, mid, high, low, mid, high, zero, zero], axis=0)


def tile_matrix():
    row = lax.broadcasted_iota(jnp.int32, (16, 128), 0)
    lane = lax.broadcasted_iota(jnp.int32, (16, 128), 1)
    return jnp.where(lane % 16 == row, 1.0, 0.0).astype(F32)


def widened(x, lanes):
    return jnp.concatenate([x, jnp.zeros((x.shape[0], lanes - x.shape[1]), x.dtype)], axis=1)


def lane_window(x, start, width):
    total = x.shape[1]
    if start:
        x = pltpu.roll(x, total - start, 1)
    return x[:, :width]


def at_lanes(x, start):
    return pltpu.roll(x, start, 1) if start else x


def blocks_kernel(coarse_hbm, blocks, coarse, wide, arrived):
    load = pltpu.make_async_copy(coarse_hbm, coarse, arrived.at[0])
    load.start()
    wide[...] = jnp.zeros_like(wide)
    load.wait()
    wide[0:3, :] = coarse[...]
    near = lax.broadcasted_iota(jnp.int32, (8, 128), 1) < 16
    row = lax.broadcasted_iota(jnp.int32, (8, 128), 0)
    unknowns = wide.shape[1]
    grid_rows = blocks.shape[0] // 8
    row_unknowns = unknowns // grid_rows
    for i in range(grid_rows):
        first = row_unknowns * (i - 1)
        span = min(unknowns, 384)
        start = min(max(first // 128, 0) * 128, unknowns - span)
        piece = wide[:, start : start + span]
        if first != start:
            piece = pltpu.roll(piece, (start - first) % span, 1)
        if span < 256:
            piece = widened(piece, 256)
        others = jnp.where(near, piece[:, 128:256], 0.0)
        others = others[0:1] + pltpu.roll(others, 16, 1)[1:2] + pltpu.roll(others, 32, 1)[2:3]
        blocks[8 * i : 8 * i + 8, :] = jnp.where(row == 6, others, pltpu.roll(piece[:, 0:128], 3, 0))


def prepare_kernel(
    count_hbm, slots_hbm, mult_hbm, modes_hbm, schur_hbm,
    place, pick_schur, mode_rows, link_rows,
    buffer, slots, mult, modes, schur, count, arrived,
):
    copies = [
        pltpu.make_async_copy(source, target, arrived.at[n])
        for n, (source, target) in enumerate(
            (
                (count_hbm, count), (slots_hbm, slots), (mult_hbm, mult), (modes_hbm, modes),
                (schur_hbm, schur),
            )
        )
    ]
    for copy in copies:
        copy.start()
    width = slots.shape[1]
    total = 4 * width
    buffer[...] = jnp.zeros_like(buffer)
    lane = lax.broadcasted_iota(jnp.int32, (1, total), 1)
    copies[0].wait()
    copies[1].wait()
    buffer[0:4, 0:width] = slots[...].astype(F32)
    raw = buffer[...]
    slot_row = jnp.zeros((1, total), F32)
    sign_row = jnp.zeros((1, total), F32)
    for f in range(4):
        inside = (lane >= width * f) & (lane < width * f + count[0, f])
        slot_row = jnp.where(inside, at_lanes(raw, width * f)[f : f + 1], slot_row)
        sign_row = jnp.where(inside, SIGNS[f], sign_row)
    copies[2].wait()
    weights = 1.0 / mult[...].astype(F32)
    buffer[...] = jnp.zeros_like(buffer)
    buffer[0:1, :] = slot_row
    buffer[1:2, :] = sign_row
    pick_value = picking(jnp.transpose(buffer[...]))
    place_value = placing(slot_row, sign_row)
    place[...] = place_value
    copies[3].wait()
    buffer[...] = jnp.zeros_like(buffer)
    for k in range(modes.shape[0]):
        buffer[k : k + 1, :] = modes[k]
    buffer[3:4, :] = weights
    rows = select_lanes(buffer[...], place_value)
    mode_rows[...] = rows
    buffer[...] = jnp.zeros_like(buffer)
    buffer[0:1, :] = slot_row
    buffer[1:2, :] = sign_row
    buffer[2:3, :] = weights
    buffer[3:4, :] = jnp.abs(rows[3:4])
    link_rows[...] = buffer[...]
    copies[4].wait()
    pick_schur[...] = dot(pick_value, schur[...]).astype(BF16)


def placing(slot_row, sign_row):
    total = slot_row.shape[1]
    down = lax.broadcasted_iota(jnp.int32, (total, total), 0).astype(F32)
    return jnp.where(down == slot_row, sign_row, 0.0).astype(BF16)


def picking(cols):
    total = cols.shape[0]
    across = lax.broadcasted_iota(jnp.int32, (total, total), 1).astype(F32)
    return jnp.where(across == cols[:, 0:1], cols[:, 1:2], 0.0).astype(BF16)


def precond_kernel(
    odd_x, odd_y, gap_down, gap_right, above, left, place, pick_schur, link_rows, mode_rows, saved,
    first_x, second_x, first_y, second_y, own, residual,
):
    width = above.shape[0]
    total = 4 * width
    columns = jnp.transpose(link_rows[...])
    links = jnp.concatenate([above[...], gap_down[...], left[...], gap_right[...]], axis=0)
    spread = select_rows(place[...], links)
    weighted = (columns[:, 2:3] * spread).astype(BF16)
    own[...] = columns[:, 3:4] * dot(pick_schur[...], weighted)
    for face, start, msg in (
        (1 - odd_x[0], 0, first_x),
        (odd_x[0], 0, second_x),
        (3 - odd_y[0], width, first_y),
        (2 + odd_y[0], width, second_y),
    ):
        msg[0:width, :] = own[pl.ds(pl.multiple_of(width * face, 8), width), :]
        rows = pltpu.roll(mode_rows[...], jnp.where(face == 0, 0, total - width * face), 1)
        msg[width : width + 8, :] = rows[:, 0:128]
        msg[width + 8 : width + 16, :] = rows[:, 128:256]
        rows = lane_window(saved[...], start, 256)
        msg[width + 16 : width + 32, :] = rows[:, 0:128]
        msg[width + 32 : width + 48, :] = rows[:, 128:256]
    residual[0:width, :] = jnp.where(columns[width : 2 * width, 1:2] != 0.0, gap_down[...], 0.0)
    residual[width:, :] = jnp.where(columns[3 * width :, 1:2] != 0.0, gap_right[...], 0.0)


def four_neighbours(odd_x, odd_y, first_x, second_x, first_y, second_y):
    even_x = odd_x[0] == 0
    even_y = odd_y[0] == 0
    return (
        jnp.where(even_x, second_x, first_x),
        jnp.where(even_x, first_x, second_x),
        jnp.where(even_y, second_y, first_y),
        jnp.where(even_y, first_y, second_y),
    )


def flex_kernel(link_rows, flex_hbm, pick_flex_hbm, flex, pick_flex, arrived):
    load = pltpu.make_async_copy(flex_hbm, flex, arrived.at[0])
    load.start()
    pick_value = picking(jnp.transpose(link_rows[...]))
    load.wait()
    pick_flex[...] = dot(pick_value, flex[...]).astype(BF16)
    store = pltpu.make_async_copy(pick_flex, pick_flex_hbm, arrived.at[1])
    store.start()
    store.wait()


def coarse_in_kernel(
    odd_x, odd_y, own, first_x, second_x, first_y, second_y, mode_rows, blocks, precond, coarse
):
    width = own.shape[0] // 4
    full = own[...] + jnp.concatenate(
        four_neighbours(
            odd_x, odd_y, first_x[0:width], second_x[0:width], first_y[0:width], second_y[0:width]
        ),
        axis=0,
    )
    precond[...] = full
    rows = dot_exact(mode_rows[...], full)
    rows = jnp.where(lax.broadcasted_iota(jnp.int32, rows.shape, 0) < 3, rows, 0.0)
    for i in range(coarse.shape[0] // 8):
        coarse[8 * i : 8 * i + 8, :] = rows + blocks[8 * i : 8 * i + 8]


def tables_kernel(
    odd_x, odd_y, first_x, second_x, first_y, second_y,
    mode_rows, link_rows, place, saved, images, residual, precond, pick_flex_hbm,
    mode_six, search_rows, base, mode_forms,
    pick_flex, arrived,
):
    load = pltpu.make_async_copy(pick_flex_hbm, pick_flex, arrived.at[0])
    load.start()
    total = mode_rows.shape[1]
    width = total // 4
    near = lax.broadcasted_iota(jnp.int32, (1, 256), 1) < width
    messages = four_neighbours(
        odd_x, odd_y, first_x[width:], second_x[width:], first_y[width:], second_y[width:]
    )
    used = link_rows[1:2, :] != 0.0
    row = lax.broadcasted_iota(jnp.int32, (16, total), 0)
    mine = jnp.concatenate([mode_rows[...], jnp.zeros((8, total), F32)], axis=0)
    modes = jnp.where(row < 3, mine, 0.0)
    for f, msg in enumerate(messages):
        theirs = jnp.concatenate([msg[0:8], msg[8:16]], axis=1)
        theirs = at_lanes(widened(jnp.where(near, theirs, 0.0), total), width * f)
        theirs = jnp.concatenate([theirs, jnp.zeros((8, total), F32)], axis=0)
        theirs = jnp.where(row < 3, theirs, 0.0)
        modes = modes + pltpu.roll(theirs, 3 * (1 + f), 0)
    modes = jnp.where(used, modes, 0.0)
    modes_tiled = tiled_columns(modes)
    mode_six[...] = six_left(modes_tiled)
    search = jnp.zeros((16, total), F32)
    for f in range(4):
        if f % 2 == 0:
            piece = jnp.concatenate([messages[f][16:32], messages[f][32:48]], axis=1)
        else:
            piece = lane_window(saved[...], 0 if f == 1 else width, 256)
        search = search + at_lanes(widened(jnp.where(near, piece, 0.0), total), width * f)
    search = jnp.where(used, search, 0.0)
    search_rows[...] = search
    lanes = lax.broadcasted_iota(jnp.int32, (16, total), 1)
    image = widened(images[...], total)
    image = jnp.where(
        (lanes >= width) & (lanes < 2 * width),
        at_lanes(image, width),
        jnp.where(lanes >= 3 * width, at_lanes(image, 2 * width), 0.0),
    )
    load.wait()
    flexed = select_lanes(jnp.concatenate([search, modes], axis=0), pick_flex[...])
    flexed = select_lanes(flexed, place[...])
    forms = jnp.concatenate([image, flexed], axis=0)
    full = precond[...]
    base[0:48, :] = dot_exact(forms, full)
    mode_forms[...] = six_left(dot_exact(forms, modes_tiled))
    high, mid, _ = split3(full)
    slots = dot(place[...], jnp.concatenate([high, mid], axis=1))
    high, mid, _ = split3(slots[:, :128] + slots[:, 128:])
    applied = dot(pick_flex[...], jnp.concatenate([high, mid], axis=1))
    square = jnp.sum(full * (applied[:, :128] + applied[:, 128:]), axis=0, keepdims=True)
    products = dot_exact(dot_exact_nt(flexed[0:16], search), tile_matrix())
    group = lax.broadcasted_iota(jnp.int32, (16, 128), 1) // 16
    part = lax.broadcasted_iota(jnp.int32, (16, 128), 0)
    products = jnp.where(group == part % 8, products, 0.0)
    energy = jnp.sum(residual[0:width] * full[width : 2 * width], axis=0, keepdims=True) + jnp.sum(
        residual[width:] * full[3 * width :], axis=0, keepdims=True
    )
    base[48:56, :] = jnp.concatenate(
        [
            energy,
            square,
            jnp.sum(products[0:8], axis=0, keepdims=True),
            jnp.sum(products[8:16], axis=0, keepdims=True),
            jnp.zeros((4, 128), F32),
        ],
        axis=0,
    )


def coarse_kernel(gathered, parts):
    arrived = gathered[...]
    height = arrived.shape[0]
    row = lax.broadcasted_iota(jnp.int32, arrived.shape, 0) % 8
    lane = lax.broadcasted_iota(jnp.int32, arrived.shape, 1)
    coarse_in = jnp.where(row < 3, arrived, 0.0)
    main = jnp.where(row < 3, pltpu.roll(arrived, height - 3, 0), 0.0)
    others = jnp.zeros_like(arrived)
    for k in range(3):
        moved = pltpu.roll(arrived, height - (6 - k), 0)
        if k:
            moved = pltpu.roll(moved, 128 - 16 * k, 1)
        others = others + jnp.where((row == k) & (lane < 16), moved, 0.0)
    product = lax.dot_general(
        jnp.concatenate([main, others], axis=1), coarse_in, (((0,), (0,)), ((), ())),
        precision=HIGHEST, preferred_element_type=F32,
    )
    total = parts.shape[0]
    count = total // 16
    row = lax.broadcasted_iota(jnp.int32, (total, 1), 0)
    j = row >> 4
    part = ((row & 15) * 11) >> 5
    mode = (row & 15) - 3 * part
    down = jnp.where(part == 1, -1, jnp.where(part == 2, 1, 0))
    j = j + jnp.where(part == 3, -1, jnp.where(part == 4, 1, 0))
    valid = (part < 5) & (j >= 0) & (j < count)
    wanted = jnp.where(valid, ((down + 1) * count + j) * 3 + mode, -1)
    at = lax.broadcasted_iota(jnp.int32, (total, 256), 1)
    parts[...] = select_rows(jnp.where(at == wanted, 1.0, 0.0).astype(BF16), product)


def block_sum(ref, height):
    out = ref[0:height]
    for j in range(1, ref.shape[0] // height):
        out = out + ref[height * j : height * j + height]
    return out


def project_kernel(chunk, arrived, base, mode_forms, amplitudes, partial):
    y = block_sum(arrived, 16)
    amplitudes[...] = y
    moved = dot(mode_forms[...], six_right(y))
    linear = base[0:32] - moved[0:32]
    square = jnp.sum(y * (moved[32:48] - 2.0 * base[32:48]), axis=0, keepdims=True)
    row = lax.broadcasted_iota(jnp.int32, (8, 128), 0)
    last = base[48:56] + jnp.where(row == 1, square, 0.0)
    padding = jnp.zeros((partial.shape[0] // 2 - 40, 128), F32)
    full = jnp.concatenate([linear, last, padding], axis=0)
    for j in range(partial.shape[0] // chunk):
        at = chunk * (j // 2)
        partial[chunk * j : chunk * j + chunk, :] = full[at : at + chunk]


def own_rows(x, width):
    return jnp.concatenate([x[width : 2 * width], x[3 * width :]], axis=0)


def lift_kernel(
    amplitudes, precond, mode_six, search_rows, link_rows,
    slot_values, slot_six, link_values, link_six,
):
    links = precond[...] - dot(mode_six[...], six_right(amplitudes[...]))
    width = links.shape[0] // 4
    link_values[...] = own_rows(links, width)
    search = search_rows[...]
    link_six[...] = six_left(own_rows(tiled_columns(search), width))
    place = placing(link_rows[0:1], link_rows[1:2])
    slot_values[...] = select_rows(place, links)
    parts = dot_nt(jnp.concatenate(split3(search), axis=0), place)
    slot_six[...] = six_left(tiled_columns(parts[0:16] + (parts[16:32] + parts[32:48])))


def spread_sum_kernel(height, arrived, partial):
    out = block_sum(arrived, height)
    for i in range(partial.shape[0] // height):
        partial[height * i : height * i + height, :] = out


def search_kernel(sums, slot_values, slot_six, pick_flex, up_msg, left_msg, own):
    width = up_msg.shape[0]
    lifted = slot_values[...] - dot(slot_six[...], six_right(sums[0:16]))
    image = dot(pick_flex[...], lifted.astype(BF16))
    up_msg[...] = image[0:width]
    left_msg[...] = image[2 * width : 3 * width]
    own[...] = own_rows(image, width)


def multiply_kernel(sums, link_values, link_six, multipliers, step):
    intersect = sums[0:16]
    cross = sums[16:32]
    energy = sums[32:33]
    square = sums[33:34]
    group = lax.broadcasted_iota(jnp.int32, (16, 128), 1) // 16
    part = lax.broadcasted_iota(jnp.int32, (16, 128), 0)
    packed = jnp.where(part < 8, sums[34:35], sums[35:36])
    packed = jnp.where(group == part % 8, packed, 0.0)
    products = dot_exact(packed, jnp.concatenate([intersect] * 8, axis=0))
    curvature = square + jnp.sum(intersect * (products - 2.0 * cross), axis=0, keepdims=True)
    size = energy / curvature
    step[...] = jnp.broadcast_to(size, step.shape)
    multipliers[...] = size * (link_values[...] - dot(link_six[...], six_right(intersect)))


def residual_kernel(before, own, below, right, step, residual):
    width = below.shape[0]
    size = step[0:1]
    residual[0:width, :] = before[0:width] - size * (own[0:width] + below[...])
    residual[width:, :] = before[width:] - size * (own[width:] + right[...])


VMEM_LIMIT = 24 * 1024 * 1024
VMEM = pl.BlockSpec(memory_space=pltpu.VMEM)
SMEM = pl.BlockSpec(memory_space=pltpu.SMEM)
HBM = pl.BlockSpec(memory_space=pltpu.HBM)


def call(kernel, inputs, outputs, scalars=0, remote=0, scratch=(), copies=0, hbm_out=(), flops=0):
    out_specs = tuple(HBM if n in hbm_out else VMEM for n in range(len(outputs)))
    outputs = tuple(
        pltpu.HBM(shape, dtype)
        if n in hbm_out
        else jax.ShapeDtypeStruct(shape, dtype)
        for n, (shape, dtype) in enumerate(outputs)
    )
    local = len(inputs) - remote
    inputs = tuple(
        x if n < local else pltpu.with_memory_space_constraint(x, pltpu.HBM)
        for n, x in enumerate(inputs)
    )
    scratch = [
        entry if not isinstance(entry, tuple) else pltpu.VMEM(*entry) for entry in scratch
    ]
    if copies:
        scratch.append(pltpu.SemaphoreType.DMA((copies,)))
    return pl.pallas_call(
        kernel,
        out_shape=outputs,
        in_specs=[SMEM] * scalars + [VMEM] * (len(inputs) - scalars - remote) + [HBM] * remote,
        out_specs=out_specs,
        scratch_shapes=scratch,
        cost_estimate=pl.CostEstimate(flops=flops, transcendentals=0, bytes_accessed=0),
        compiler_params=pltpu.CompilerParams(vmem_limit_bytes=VMEM_LIMIT),
    )(*inputs)


def step(
    gap_load, flexibility, schur_blocks, body_modes, coarse_inverse,
    saved_search, saved_images, face_slots, face_count, multiplicity,
):
    rows = lax.axis_size(GX)
    columns = lax.axis_size(GY)
    gap = gap_load[0, 0]
    flex = flexibility[0, 0]
    modes = jnp.transpose(body_modes, (0, 2, 1, 3))[0]
    saved = saved_search[0, 0]
    images = saved_images[0, 0]
    slots = face_slots[0, 0]
    count = face_count[0]
    width = slots.shape[1]
    total = 4 * width
    cases = gap.shape[1]
    unknowns = coarse_inverse.shape[1]
    big = (total, total)
    cube = 2 * total**3
    gap_down = gap[:width]
    gap_right = gap[width:]
    above = shifted(gap_down, GX, 1)
    left = shifted(gap_right, GY, 1)
    place, pick_schur, mode_rows, link_rows = call(
        prepare_kernel,
        (count, slots, multiplicity[0], modes, schur_blocks[0, 0]),
        (
            (big, BF16), (big, BF16), ((8, total), F32), ((8, total), F32),
        ),
        remote=5,
        scratch=(
            ((8, total), F32), (slots.shape, jnp.int32), ((1, total), jnp.int32), (modes.shape, F32),
            (big, BF16), pltpu.SMEM((1, 4), jnp.int32),
        ),
        copies=5,
        flops=cube,
    )
    odd_x = (lax.axis_index(GX) % 2).reshape(1)
    odd_y = (lax.axis_index(GY) % 2).reshape(1)
    first_x, second_x, first_y, second_y, own, residual = call(
        precond_kernel,
        (odd_x, odd_y, gap_down, gap_right, above, left, place, pick_schur, link_rows, mode_rows, saved),
        (((width + 48, cases), F32),) * 4 + (((total, cases), F32), ((2 * width, cases), F32)),
        scalars=2,
        flops=cube // 2,
    )
    first_x = swapped(first_x, GX, 0)
    second_x = swapped(second_x, GX, 1)
    first_y = swapped(first_y, GY, 0)
    second_y = swapped(second_y, GY, 1)
    messages = (first_x, second_x, first_y, second_y)
    (blocks,) = call(
        blocks_kernel,
        (coarse_inverse,),
        (((8 * rows, 128), F32),),
        remote=1,
        scratch=((coarse_inverse.shape, F32), ((8, unknowns), F32)),
        copies=1,
        flops=cube // 64,
    )
    precond, coarse_in = call(
        coarse_in_kernel,
        (odd_x, odd_y, own, *messages, mode_rows, blocks),
        (((total, cases), F32), ((8 * rows, cases), F32)),
        scalars=2,
        flops=cube // 16,
    )
    gathered = lax.all_to_all(coarse_in, GX, 0, 0, tiled=True)
    (pick_flex,) = call(
        flex_kernel,
        (link_rows, flex),
        ((big, BF16),),
        remote=1,
        scratch=((big, BF16), (big, BF16)),
        copies=2,
        hbm_out=(0,),
        flops=cube,
    )
    (parts,) = call(coarse_kernel, (gathered,), (((16 * columns, cases), F32),), flops=cube // 8)
    parts = lax.all_to_all(parts, GY, 0, 0, tiled=True)
    mode_six, search_rows, base, mode_forms = call(
        tables_kernel,
        (
            odd_x, odd_y, *messages, mode_rows, link_rows, place, saved, images, residual, precond,
            pick_flex,
        ),
        (((total, 128), BF16), ((16, total), F32), ((56, cases), F32), ((48, 128), BF16)),
        scalars=2,
        remote=1,
        scratch=((big, BF16),),
        copies=1,
        flops=cube,
    )
    pairs = columns // 2
    chunk = -(-(-(-40 // pairs)) // 8) * 8
    amplitudes, partial = call(
        functools.partial(project_kernel, chunk),
        (parts, base, mode_forms),
        (((16, cases), F32), ((chunk * columns, cases), F32)),
        flops=cube // 64,
    )
    slot_values, slot_six, link_values, link_six = call(
        lift_kernel,
        (amplitudes, precond, mode_six, search_rows, link_rows),
        (
            ((total, cases), F32), ((total, 128), BF16), ((2 * width, cases), F32),
            ((2 * width, 128), BF16),
        ),
        flops=cube,
    )
    for axis, following in ((GY, rows), (GX, pairs)):
        partial = lax.all_to_all(partial, axis, 0, 0, tiled=True)
        (partial,) = call(
            functools.partial(spread_sum_kernel, chunk),
            (partial,),
            (((chunk * following, cases), F32),),
            flops=cube // 64,
        )
    sums = lax.all_to_all(partial, GY[0], 0, 0, tiled=True)
    up_msg, left_msg, own = call(
        search_kernel,
        (sums, slot_values, slot_six, pick_flex),
        (((width, cases), F32), ((width, cases), F32), ((2 * width, cases), F32)),
        flops=cube // 2,
    )
    from_below = shifted(up_msg, GX, -1)
    from_right = shifted(left_msg, GY, -1)
    multipliers, step = call(
        multiply_kernel,
        (sums, link_values, link_six),
        (((2 * width, cases), F32), ((8, cases), F32)),
        flops=cube // 64,
    )
    (residual,) = call(
        residual_kernel,
        (residual, own, from_below, from_right, step),
        (((2 * width, cases), F32),),
        flops=cube // 64,
    )
    return (multipliers[None, None], residual[None, None])


def split_shape(mesh):
    rows, columns = (mesh.devices.shape[0], mesh.devices.shape[1])
    inner = 4 if rows % 4 == 0 and rows > 4 else 2
    return (rows // inner, inner, columns // 2, 2)


def solution(mesh):
    split = Mesh(mesh.devices.reshape(split_shape(mesh)), GX_GY)
    placed = (
        P(GX, GY, None, None),
        P(GX, GY, None, None),
        P(GX, GY, None, None),
        P(GX, GY, None, None),
        P(GX_GY, None),
        P(GX, GY, None, None),
        P(GX, GY, None, None),
        P(GX, GY, None, None),
        P(GX, GY, None),
        P(GX, GY, None),
    )
    return jax.shard_map(
        step,
        mesh=split,
        in_specs=placed,
        out_specs=(P(GX, GY, None, None), P(GX, GY, None, None)),
        check_vma=False,
    )
```
